256 devices in a mesh: real: 4 (over y, x), row: 64 (over z, core).
Axes of the slice: x: 2, y: 2, z: 32, core: 2. Of those that a mesh axis runs over, the one named last changes fastest.
The devices are a block of a 4x8x32 slice.
Arguments:
- site_tensor: float32 [256, 2, 256, 256], P(('real', 'row')), parts along dimension 0, may hold values from -20 to 20
- left_env: float32 [256, 14, 256, 256], P(('real', 'row')), parts along dimension 0, may hold values from -10 to 10
- right_env: float32 [256, 14, 256, 256], P(('real', 'row')), parts along dimension 0, may hold values from -10 to 10
- sector_size: int32 [256], P('real'), parts along dimension 0, may hold values from 64 to 256
Outputs:
- left_out: float32 [256, 2, 256, 256], P(('real', 'row')), parts along dimension 0
- bond_out: float32 [256, 256, 256], P(('real', 'row')), parts along dimension 0
The draws below stay inside these ranges and needn't reach their ends.
There are 4 independent parts, one for each index of `real`. The reference program is written for one: setup_inputs(seed, part) draws one part's arguments, and reference() takes and returns one part's arrays. A program takes and returns all parts, laid end to end along the dimension named above; each array names one. Nothing has to cross between parts.
All inputs are finite; a program needn't handle non-finite values.
Results may differ from the reference program's by a relative error of at most 0.00005.
Values sent between devices are 32-bit elements; how exact they have to be, the bound alone decides.
A program may use at most 64 MiB of HBM per device.

```python
import jax
import jax.numpy as jnp
from jax import lax

SEC = 256
W_DN = 4
W_UP = 4
W = 14
SECTORS = 64


def sector_ramp(total_rise):
    position = jnp.arange(SECTORS, dtype=jnp.float32) / max(SECTORS - 1, 1)
    return jnp.exp(jnp.log(total_rise) * position)


def draw_site_tensor(key, part):
    key_noise, key_scale = jax.random.split(jax.random.fold_in(key, 11))
    random_part = jnp.clip(jax.random.normal(key_noise, (SECTORS, 2, SEC, SEC), jnp.float32), -6.0, 6.0)
    column_scale = jnp.exp(jnp.clip(0.2 * jax.random.normal(key_scale, (SECTORS, 2, 1, SEC), jnp.float32), -0.8, 0.8))
    ramp = jnp.sqrt(sector_ramp(3.0))
    random_part = random_part * SEC ** (-0.5)
    identity = jnp.eye(SEC, dtype=jnp.float32)
    upper_block = identity[None] + 0.35 * random_part[:, 0]
    lower_block = 0.7 * random_part[:, 1]
    return jnp.stack([upper_block, lower_block], 1) * column_scale * ramp[:, None, None, None]


def environment_noise(key):
    noise = jnp.clip(jax.random.normal(key, (SECTORS, W, SEC, SEC), jnp.float32), -6.0, 6.0)
    return noise * SEC ** (-0.5)


def draw_left_env(key, part):
    key_noise, key_field = jax.random.split(jax.random.fold_in(key, 23))
    noise = environment_noise(key_noise)
    rough = jnp.exp(jax.random.uniform(key_field, (SECTORS, SEC), jnp.float32, jnp.log(0.5), jnp.log(2.0)))
    ramp = sector_ramp(3.0)
    field = rough * ramp[:, None]
    identity = jnp.eye(SEC, dtype=jnp.float32)
    onsite = field[:, :, None] * identity[None]
    return noise.at[:, W - 1].add(onsite)


def draw_right_env(key, part):
    noise = environment_noise(jax.random.fold_in(key, 37))
    identity = jnp.eye(SEC, dtype=jnp.float32)
    return noise.at[:, W - 1].add(identity[None])


def with_ends(values, own_key, least, high):
    dims = values.shape
    index_at = [jax.random.randint(jax.random.fold_in(own_key, axis), (), 0, dims[axis]) for axis in range(len(dims))]
    values = values.at[tuple(index_at)].set(least)
    longest = dims.index(max(dims))
    index_at[longest] = (index_at[longest] + 1) % dims[longest]
    return values.at[tuple(index_at)].set(high)


def setup_inputs(seed: int = 0, part: int = 0) -> dict:
    seeds = jax.random.split(jax.random.key(seed), 5)
    part_keys = jax.random.split(jax.random.fold_in(seeds[4], part), 5)
    site_tensor = draw_site_tensor(jax.random.fold_in(jax.random.fold_in(seeds[4], part), 71), part)
    left_env = draw_left_env(jax.random.fold_in(jax.random.fold_in(seeds[4], part), 71), part)
    right_env = draw_right_env(jax.random.fold_in(jax.random.fold_in(seeds[4], part), 71), part)
    sector_size = with_ends(jax.random.randint(part_keys[3], (SECTORS,), SEC // 4, SEC + 1), jax.random.fold_in(part_keys[3], 1), SEC // 4, SEC).astype(jnp.int32)
    return {"site_tensor": site_tensor, "left_env": left_env, "right_env": right_env, "sector_size": sector_size}


highest = lax.Precision.HIGHEST
time_step = 0.15

def solve_rows(factor, stacked):
    return jax.scipy.linalg.solve_triangular(factor, stacked.T, lower=True).T

def apply_bond(operand, left_env, right_env, mask_pair):
    products = jnp.einsum('sik,sakl->sail', operand, right_env, precision=highest)
    empty_block = jnp.zeros_like(products[:1])
    down_terms = jnp.concatenate([empty_block[:, :W_DN], products[:-1, :W_DN]], 0)
    upper_terms = jnp.concatenate([products[1:, W_DN:W_DN + W_UP], empty_block[:, W_DN:W_DN + W_UP]], 0)
    combined = jnp.concatenate([down_terms, upper_terms, products[:, W_DN + W_UP:]], 1)
    return jnp.einsum('saij,sajl->sil', left_env, combined, precision=highest) * mask_pair

def reference(site_tensor, left_env, right_env, sector_size):
    live_mask = (jnp.arange(SEC, dtype=jnp.int32)[None, :] < sector_size[:, None]).astype(jnp.float32)
    row_mask = live_mask[:, :, None]
    col_mask = live_mask[:, None, :]
    mask_pair = row_mask * col_mask
    upper_block = site_tensor[:, 0] * mask_pair
    lower_source = site_tensor[:, 1] * row_mask
    lower_block = jnp.concatenate([jnp.zeros_like(lower_source[:1]), lower_source[:-1]], 0) * col_mask
    stacked = jnp.concatenate([upper_block, lower_block], 1)
    identity = jnp.eye(SEC, dtype=jnp.float32)
    gram_matrix = jnp.einsum('sij,sik->sjk', stacked, stacked, precision=highest) + identity[None] * (1.0 - live_mask)[:, None, :]
    factor = jnp.linalg.cholesky(gram_matrix)
    orthonormal = jax.vmap(solve_rows)(factor, stacked)
    moved_back = jnp.concatenate([orthonormal[1:, SEC:], jnp.zeros_like(orthonormal[:1, SEC:])], 0)
    left_out = jnp.stack([orthonormal[:, :SEC], moved_back], 1)
    bond_matrix = jnp.swapaxes(factor, 1, 2) * mask_pair
    start_norm = jnp.sum(bond_matrix * bond_matrix)
    applied = apply_bond(bond_matrix, left_env, right_env, mask_pair)
    energy = jnp.sum(bond_matrix * applied) / start_norm
    shifted = applied - energy * bond_matrix
    second = apply_bond(shifted, left_env, right_env, mask_pair) - energy * shifted
    evolved = bond_matrix + time_step * shifted + 0.5 * time_step * time_step * second
    final_norm = jnp.sum(evolved * evolved)
    return (left_out, evolved * jnp.sqrt(start_norm / final_norm))
```

```python
import functools

import jax
import jax.numpy as jnp
from jax import lax
from jax.experimental import pallas as pl
from jax.experimental.pallas import tpu as pltpu
from jax.sharding import PartitionSpec as P

MESH = pl.DeviceIdType.MESH
W_DN = 4
W_UP = 4
HALO = W_DN + W_UP
TAU = 0.15
BLK = 64
highest = lax.Precision.HIGHEST
f32 = jnp.float32
bf16 = jnp.bfloat16


def across_lanes(tile, lane):
    return jnp.broadcast_to(tile[:, lane : lane + 1], tile.shape)


def across_rows(tile, row):
    return jnp.broadcast_to(tile[row : row + 1, :], tile.shape)


def eliminate(tiles, first):
    sub = lax.broadcasted_iota(jnp.int32, (8, 128), 0)
    count = len(tiles)
    tiles = list(tiles)
    for g in range(count):
        cols = {v: [across_lanes(tiles[v], first + 8 * g + j) for j in range(8)] for v in range(g, count)}
        pivots = None
        for j in range(8):
            pivot = across_rows(cols[g][j], j)
            inverse = 1.0 / pivot
            pivots = pivot if pivots is None else jnp.where(sub == j, pivot, pivots)
            row = across_rows(tiles[g], j) * inverse
            heads = [across_rows(cols[g][k], j) * inverse for k in range(j + 1, 8)]
            below = jnp.where(sub > j, cols[g][j], 0.0)
            for v in range(g, count):
                factor = below if v == g else cols[v][j]
                for k in range(j + 1, 8):
                    cols[v][k] = cols[v][k] - factor * heads[k - j - 1]
                tiles[v] = tiles[v] - factor * row
        tiles[g] = tiles[g] * lax.rsqrt(pivots)
    return tiles


def dot(a, b, dims=((1,), (0,)), precision=None):
    return lax.dot_general(a, b, (dims, ((), ())), precision=precision, preferred_element_type=f32)


def split(x):
    high = x.astype(bf16)
    return high, (x - high.astype(f32)).astype(bf16)


def dot3(ah, al, bh, bl):
    return dot(ah, bh) + dot(ah, bl) + dot(al, bh)


def factorize(gram, upper, bond, diag_inverse, mask_pair, done):
    size = gram.shape[0]
    for k in range(size // BLK):
        r0 = k * BLK
        c0 = r0 // 128 * 128
        first = r0 - c0
        lane = lax.broadcasted_iota(jnp.int32, (8, 128), 1)
        sub = lax.broadcasted_iota(jnp.int32, (8, 128), 0)
        in_block = (lane >= first) & (lane < first + BLK)
        other = BLK - first
        tiles = []
        for g in range(BLK // 8):
            unit = (lane - other == sub + 8 * g).astype(f32)
            tiles.append(jnp.where(in_block, gram[r0 + 8 * g : r0 + 8 * g + 8, c0 : c0 + 128], unit))
        tiles = eliminate(tiles, first)
        both = jnp.concatenate(tiles, axis=0)
        lane_b = lax.broadcasted_iota(jnp.int32, (BLK, 128), 1)
        row_b = lax.broadcasted_iota(jnp.int32, (BLK, 128), 0)
        in_b = (lane_b >= first) & (lane_b < first + BLK)
        inverse = jnp.where(in_b, 0.0, both)
        diag_inverse[k] = inverse
        rows = gram[r0 : r0 + BLK, c0:]
        panel = dot(inverse, jnp.concatenate([rows, rows], axis=0), precision=highest)
        head = jnp.where(in_b, both, panel[:, :128])
        head = jnp.where(lane_b - first >= row_b, head, 0.0)
        panel = jnp.concatenate([head, panel[:, 128:]], axis=1) if panel.shape[1] > 128 else head
        upper[r0 : r0 + BLK, c0:] = panel
        bond[r0 : r0 + BLK, c0:] = jnp.where(mask_pair(r0, BLK, c0), panel, 0.0)
        done(k, r0, c0)
        if r0 + BLK < size:
            t0 = (r0 + BLK) // 128 * 128
            tail = panel[:, t0 - c0 :]
            gram[t0:, t0:] = gram[t0:, t0:] - dot(tail, tail, ((0,), (0,)), precision=highest)


def kernel(
    n, sizes, site, left_env, right_env, left_out, bond_out,
    site_v, low_v, left_f, right_f, down_f, up_f, left_h, left_l, right_h, right_l,
    gram, upper, bond, inv, halo_m, halo_p, app, app_m, app_p, second, mix_h, mix_l,
    ortho_v, result_v, mine, slots, partner,
    local_sem, out_sem, site_sem, env_sem, bond_sem, app_sem, low_sem, far_sem, pair_sem, known_sem,
):
    me = lax.axis_index("row")
    size = site.shape[-1]
    width = left_env.shape[1]
    chips = n // 2

    def other(step):
        return {"row": lax.rem(me + step + n, n)}

    after, before = other(1), other(-1)
    pair = {"row": me + 1 - 2 * lax.rem(me, 2)}

    def remote(src, dst, sems, target):
        return pltpu.make_async_remote_copy(
            src_ref=src, dst_ref=dst, send_sem=sems.at[0], recv_sem=sems.at[1], device_id=target, device_id_type=MESH
        )

    load_site = pltpu.make_async_copy(site.at[0], site_v, local_sem.at[0])
    load_left = pltpu.make_async_copy(left_env.at[0], left_f, local_sem.at[1])
    load_right = pltpu.make_async_copy(right_env.at[0, pl.ds(HALO, width - HALO)], right_f, local_sem.at[2])
    load_site.start()
    load_left.start()
    load_right.start()

    barrier = pltpu.get_barrier_semaphore()
    for step in (1, -1, 2, -2):
        pl.semaphore_signal(barrier, inc=1, device_id=other(step), device_id_type=MESH)
    pl.semaphore_wait(barrier, 4)

    move_site = remote(site.at[0, 1], low_v, site_sem, after)
    move_down = remote(right_env.at[0, pl.ds(0, W_DN)], down_f, env_sem.at[0], after)
    move_up = remote(right_env.at[0, pl.ds(W_DN, W_UP)], up_f, env_sem.at[1], before)
    move_site.start()
    move_down.start()
    move_up.start()

    rounds = []
    reach = 1
    while 2 * reach <= chips // 2:
        rounds.append(reach)
        reach *= 2

    def greet(i):
        if i < len(rounds):
            for step in (2 * rounds[i], -2 * rounds[i]):
                pl.semaphore_signal(known_sem.at[i], inc=1, device_id=other(step), device_id_type=MESH)

    def greeted(i):
        if i < len(rounds):
            pl.semaphore_wait(known_sem.at[i], 2)

    greet(0)

    own_size = sizes[me]
    low_size = jnp.where(me == 0, 0, sizes[lax.rem(me + n - 1, n)])

    def mask_pair(r0, rows, c0, row_size=None):
        shape = (rows, size - c0)
        row = lax.broadcasted_iota(jnp.int32, shape, 0) + r0
        lane = lax.broadcasted_iota(jnp.int32, shape, 1) + c0
        return (row < (own_size if row_size is None else row_size)) & (lane < own_size)

    load_site.wait()
    ortho_v[0] = jnp.where(mask_pair(0, size, 0), site_v[0], 0.0)
    gram[...] = dot(ortho_v[0], ortho_v[0], ((0,), (0,)), precision=highest)

    def split_into(source, offset):
        def body(i, _):
            high, low = split(source[i])
            at = pl.ds(pl.multiple_of((i + offset) * size, size), size)
            right_h[at, :] = high
            right_l[at, :] = low
            return 0

        lax.fori_loop(0, source.shape[0], body, 0)

    load_left.wait()

    def split_left(i, _):
        high, low = split(left_f[i])
        left_h[i] = high
        left_l[i] = low
        return 0

    lax.fori_loop(0, width, split_left, 0)
    load_right.wait()
    split_into(right_f, HALO)

    move_site.wait_recv()
    ortho_v[1] = jnp.where(mask_pair(0, size, 0, low_size), low_v[...], 0.0)
    row = lax.broadcasted_iota(jnp.int32, (size, size), 0)
    lane = lax.broadcasted_iota(jnp.int32, (size, size), 1)
    dead = ((row == lane) & (row >= own_size)).astype(f32)
    gram[...] = gram[...] + dot(ortho_v[1], ortho_v[1], ((0,), (0,)), precision=highest) + dead

    sends = []

    def bond_piece(k, r0, c0):
        at = (pl.ds(r0, BLK), pl.ds(c0, size - c0))
        for side, (target, halo) in enumerate(((after, halo_m), (before, halo_p))):
            copy = remote(bond.at[at], halo.at[at], bond_sem.at[side, k], target)
            copy.start()
            sends.append(copy)
        greeted(k)
        greet(k + 1)

    bond[size // 2 :, : size // 2] = jnp.zeros((size // 2, size // 2), f32)
    factorize(gram, upper, bond, inv, mask_pair, bond_piece)
    for i in range(size // BLK, len(rounds)):
        greeted(i)
        greet(i + 1)

    def stage_one(first, last, block):
        high, low = split(block)
        for a in range(first, last):
            mixed = dot3(left_h[a], left_l[a], high, low)
            at = slice(a * size, (a + 1) * size)
            mix_h[:, at], mix_l[:, at] = split(mixed)

    def stage_two(r0, rows):
        at = slice(r0, r0 + rows)
        return dot3(mix_h[at, :], mix_l[at, :], right_h[...], right_l[...])

    stage_one(HALO, width, bond[...])
    move_down.wait_recv()
    split_into(down_f, 0)
    move_up.wait_recv()
    split_into(up_f, W_DN)
    for copy in sends:
        copy.wait_recv()

    half = size // 2

    def bond_halo(ref, valid):
        low = jnp.concatenate([jnp.zeros((half, half), f32), ref[half:, half:]], axis=1)
        return jnp.where(valid, jnp.concatenate([ref[:half, :], low], axis=0), 0.0)

    has_before = jnp.broadcast_to(me, (size, size)) > 0
    has_after = jnp.broadcast_to(me, (size, size)) < n - 1
    stage_one(0, W_DN, bond_halo(halo_m, has_before))
    stage_one(W_DN, HALO, bond_halo(halo_p, has_after))

    app_sends = []
    for part in range(2):
        r0 = part * half
        app[r0 : r0 + half, :] = jnp.where(mask_pair(r0, half, 0), TAU * stage_two(r0, half), 0.0)
        at = pl.ds(r0, half)
        for side, (target, halo) in enumerate(((after, app_m), (before, app_p))):
            copy = remote(app.at[at], halo.at[at], app_sem.at[side, part], target)
            copy.start()
            app_sends.append(copy)

    stage_one(HALO, width, app[...])
    for copy in app_sends:
        copy.wait_recv()
    stage_one(0, W_DN, jnp.where(has_before, app_m[...], 0.0))
    stage_one(W_DN, HALO, jnp.where(has_after, app_p[...], 0.0))
    second[...] = jnp.where(mask_pair(0, size, 0), (0.5 * TAU) * stage_two(0, size), 0.0)

    def total(x):
        return jnp.sum(jnp.sum(x, axis=0, keepdims=True), axis=1, keepdims=True)

    b, a, h = bond[...], app[...], second[...]
    pieces = [total(x) for x in (b * b, b * a, a * a, b * h, a * h, h * h)]
    lane_1 = lax.broadcasted_iota(jnp.int32, (1, 128), 1)
    packed = jnp.zeros((1, 128), f32)
    for i, piece in enumerate(pieces):
        packed = jnp.where(lane_1 == i, piece, packed)
    mine[0] = packed

    def far(d):
        return pltpu.make_async_remote_copy(
            src_ref=mine.at[0], dst_ref=slots.at[d - 1], send_sem=far_sem.at[0, d - 1], recv_sem=far_sem.at[1, d - 1],
            device_id={"row": lax.rem(me + 2 * d, n)}, device_id_type=MESH,
        )

    def send_far(i, _):
        d = chips // 2 + (i + 1) // 2 * (2 * (i % 2) - 1)
        far(d).start()
        return 0

    lax.fori_loop(0, chips - 1, send_far, 0)

    def ortho_rows(part):
        blocks = []
        for k in range(size // BLK):
            r0 = k * BLK
            c0 = r0 // 128 * 128
            want = ortho_v[part][:, c0 : c0 + 128]
            if k:
                done = jnp.concatenate(blocks, axis=1)
                want = want - dot(done, upper[:r0, c0 : c0 + 128], precision=highest)
            first = r0 - c0
            inverse = inv[k][:, BLK - first : 2 * BLK - first]
            blocks.append(dot(want[:, first : first + BLK], inverse, ((1,), (1,)), precision=highest))
        return jnp.concatenate(blocks, axis=1)

    result_v[1] = ortho_rows(1)
    move_low = remote(result_v.at[1], left_out.at[0, 1], low_sem, before)
    move_low.start()
    result_v[0] = ortho_rows(0)
    store_up = pltpu.make_async_copy(result_v.at[0], left_out.at[0, 0], out_sem.at[0])
    store_up.start()

    def take_far(i, _):
        far(i + 1).wait_recv()
        return 0

    lax.fori_loop(0, chips - 1, take_far, 0)
    mine[1] = mine[0] + jnp.sum(slots[...], axis=0)
    swap = remote(mine.at[1], partner, pair_sem, pair)
    swap.start()
    swap.wait_recv()
    sums = mine[1] + partner[...]
    bb, ba, aa, bh, ah, hh = (jnp.broadcast_to(sums[:, i : i + 1], (1, size)) for i in range(6))
    step = ba / bb
    weight_b = 1.0 - step + 0.5 * step * step
    weight_a = 1.0 - step
    norm = (
        weight_b * weight_b * bb + 2.0 * weight_b * weight_a * ba + weight_a * weight_a * aa
        + 2.0 * weight_b * bh + 2.0 * weight_a * ah + hh
    )
    scale = jnp.sqrt(bb / norm)
    bond_out[0] = (weight_b * bond[...] + weight_a * app[...] + second[...]) * scale

    def sent_far(i, _):
        far(i + 1).wait_send()
        return 0

    lax.fori_loop(0, chips - 1, sent_far, 0)
    for copy in (move_site, move_down, move_up, *sends, *app_sends, swap, move_low):
        copy.wait_send()
    move_low.wait_recv()
    store_up.wait()


def on_device(n, site_tensor, left_env, right_env, sector_size):
    size = site_tensor.shape[-1]
    width = left_env.shape[1]
    full = (size, size)
    hbm = pl.BlockSpec(memory_space=pl.ANY)
    chips = n // 2
    parts = size // BLK
    scratch = [
        pltpu.VMEM((2, *full), f32), pltpu.VMEM(full, f32), pltpu.VMEM((width, *full), f32),
        pltpu.VMEM((width - HALO, *full), f32), pltpu.VMEM((W_DN, *full), f32), pltpu.VMEM((W_UP, *full), f32),
        pltpu.VMEM((width, *full), bf16), pltpu.VMEM((width, *full), bf16),
        pltpu.VMEM((width * size, size), bf16), pltpu.VMEM((width * size, size), bf16),
        pltpu.VMEM(full, f32), pltpu.VMEM(full, f32), pltpu.VMEM(full, f32), pltpu.VMEM((parts, BLK, 128), f32),
        pltpu.VMEM(full, f32), pltpu.VMEM(full, f32), pltpu.VMEM(full, f32), pltpu.VMEM(full, f32),
        pltpu.VMEM(full, f32), pltpu.VMEM(full, f32),
        pltpu.VMEM((size, width * size), bf16), pltpu.VMEM((size, width * size), bf16),
        pltpu.VMEM((2, *full), f32), pltpu.VMEM((2, *full), f32),
        pltpu.VMEM((2, 1, 128), f32), pltpu.VMEM((chips - 1, 1, 128), f32), pltpu.VMEM((1, 128), f32),
        pltpu.SemaphoreType.DMA((3,)), pltpu.SemaphoreType.DMA((1,)), pltpu.SemaphoreType.DMA((2,)),
        pltpu.SemaphoreType.DMA((2, 2)), pltpu.SemaphoreType.DMA((2, parts, 2)), pltpu.SemaphoreType.DMA((2, 2, 2)),
        pltpu.SemaphoreType.DMA((2,)), pltpu.SemaphoreType.DMA((2, chips - 1)), pltpu.SemaphoreType.DMA((2,)),
        pltpu.SemaphoreType.REGULAR((max(1, chips.bit_length()),)),
    ]
    return pl.pallas_call(
        functools.partial(kernel, n),
        out_shape=(
            jax.ShapeDtypeStruct((1, 2, *full), f32),
            jax.ShapeDtypeStruct((1, *full), f32),
        ),
        in_specs=[pl.BlockSpec(memory_space=pltpu.SMEM), hbm, hbm, hbm],
        out_specs=(hbm, pl.BlockSpec(memory_space=pltpu.VMEM)),
        scratch_shapes=scratch,
        compiler_params=pltpu.CompilerParams(
            collective_id=0, has_side_effects=True, vmem_limit_bytes=60 * 1024 * 1024
        ),
    )(sector_size, site_tensor, left_env, right_env)


def solution(mesh):
    block = P(("real", "row"), None, None, None)
    return jax.shard_map(
        functools.partial(on_device, mesh.shape["row"]),
        mesh=mesh,
        in_specs=(block, block, block, P("real")),
        out_specs=(block, P(("real", "row"), None, None)),
        check_vma=False,
    )
```

```python
import functools

import jax
import jax.numpy as jnp
from jax import lax
from jax.experimental import pallas as pl
from jax.experimental.pallas import tpu as pltpu
from jax.sharding import PartitionSpec as P

MESH = pl.DeviceIdType.MESH
W_DN = 4
W_UP = 4
HALO = W_DN + W_UP
TAU = 0.15
BLK = 64
highest = lax.Precision.HIGHEST
f32 = jnp.float32
bf16 = jnp.bfloat16


def across_lanes(tile, lane):
    return jnp.broadcast_to(tile[:, lane : lane + 1], tile.shape)


def across_rows(tile, row):
    return jnp.broadcast_to(tile[row : row + 1, :], tile.shape)


def eliminate(tiles, first):
    sub = lax.broadcasted_iota(jnp.int32, (8, 128), 0)
    count = len(tiles)
    tiles = [list(tile) for tile in tiles]
    own = [across_lanes(tiles[0][0], first + j) for j in range(8)]
    for g in range(count):
        last = g + 1 == count
        ahead = [] if last else [across_lanes(tiles[g + 1][0], first + 8 * (g + 1) + j) for j in range(8)]
        cols = {v: [across_lanes(tiles[v][0], first + 8 * g + j) for j in range(8)] for v in range(g + 1, count)}
        pivots = None
        for j in range(8):
            pivot = across_rows(own[j], j)
            inverse = 1.0 / pivot
            pivots = pivot if pivots is None else jnp.where(sub == j, pivot, pivots)
            heads = {k: across_rows(own[k], j) * inverse for k in range(j + 1, 8)}
            below = jnp.where(sub > j, own[j], 0.0)
            for k in range(j + 1, 8):
                own[k] = own[k] - below * heads[k]
            rows = [across_rows(part, j) * inverse for part in tiles[g]]
            tiles[g] = [part - below * row for part, row in zip(tiles[g], rows)]
            for v in range(g + 1, count):
                factor = cols[v][j]
                for k in range(j + 1, 8):
                    cols[v][k] = cols[v][k] - factor * heads[k]
                tiles[v] = [part - factor * row for part, row in zip(tiles[v], rows)]
            if not last:
                factor = cols[g + 1][j]
                scaled = factor * inverse
                ahead = [col - factor * across_rows(scaled, k) for k, col in enumerate(ahead)]
        scale = lax.rsqrt(pivots)
        tiles[g] = [part * scale for part in tiles[g]]
        own = ahead
    return tiles


def dot(a, b, dims=((1,), (0,)), precision=None):
    return lax.dot_general(a, b, (dims, ((), ())), precision=precision, preferred_element_type=f32)


def split(x):
    high = x.astype(bf16)
    return high, (x - high.astype(f32)).astype(bf16)


def dot3(ah, al, bh, bl):
    return dot(ah, bh) + dot(ah, bl) + dot(al, bh)


def factorize(gram, upper, bond, diag_inverse, mask_pair, done):
    size = gram.shape[0]
    lane = lax.broadcasted_iota(jnp.int32, (8, 128), 1)
    sub = lax.broadcasted_iota(jnp.int32, (8, 128), 0)
    for k in range(size // BLK):
        r0 = k * BLK
        c0 = r0 // 128 * 128
        first = r0 - c0
        tiles = []
        for g in range(BLK // 8):
            at = slice(r0 + 8 * g, r0 + 8 * g + 8)
            unit = (lane == sub + 8 * g).astype(f32)
            parts = [gram[at, c : c + 128] for c in range(c0, size, 128)]
            if first:
                parts[0] = jnp.where(lane >= first, parts[0], unit)
            else:
                parts.append(unit)
            tiles.append(parts)
        tiles = eliminate(tiles, first)
        parts = [jnp.concatenate([tile[i] for tile in tiles], axis=0) for i in range(len(tiles[0]))]
        diag_inverse[k] = parts[0] if first else parts.pop()
        lane_b = lax.broadcasted_iota(jnp.int32, (BLK, 128), 1)
        row_b = lax.broadcasted_iota(jnp.int32, (BLK, 128), 0)
        parts[0] = jnp.where(lane_b - first >= row_b, parts[0], 0.0)
        panel = jnp.concatenate(parts, axis=1) if len(parts) > 1 else parts[0]
        if r0 + BLK < size:
            if not first:
                turned = jnp.transpose(parts[0])[BLK:, :]
                at = slice(r0 + BLK, r0 + 2 * BLK)
                gram[at, c0:] = gram[at, c0:] - dot(turned, panel, precision=highest)
            if len(parts) > 1:
                turned = jnp.transpose(parts[1])
                gram[c0 + 128 :, c0 + 128 :] = gram[c0 + 128 :, c0 + 128 :] - dot(turned, parts[1], precision=highest)
        upper[r0 : r0 + BLK, c0:] = panel
        bond[r0 : r0 + BLK, c0:] = jnp.where(mask_pair(r0, BLK, c0), panel, 0.0)
        done(k, r0, c0)


def kernel(
    n, sizes, site, left_env, right_env, left_out, bond_out,
    site_v, low_v, left_f, right_f, near_f, cross_f, left_h, left_l, right_h, right_l,
    gram, upper, bond, inv, halo_n, halo_c, app, app_n, app_c, second, part_v, mix_h, mix_l,
    ortho_v, result_v, mine, slots, partner,
    local_sem, out_sem, site_sem, near_sem, cross_sem, bond_sem, app_sem, low_sem, far_sem, pair_sem, known_sem,
):
    me = lax.axis_index("row")
    odd = lax.rem(me, 2)
    size = site.shape[-1]
    half = size // 2
    width = left_env.shape[1]
    own_n = width - HALO
    met_n = own_n + W_DN
    chips = n // 2

    def other(step):
        return {"row": lax.rem(me + step + n, n)}

    near, cross = other(1 - 2 * odd), other(2 * odd - 1)

    def remote(src, dst, sems, target):
        return pltpu.make_async_remote_copy(
            src_ref=src, dst_ref=dst, send_sem=sems.at[0], recv_sem=sems.at[1], device_id=target, device_id_type=MESH
        )

    load_site = pltpu.make_async_copy(site.at[0], site_v, local_sem.at[0])
    load_left = pltpu.make_async_copy(left_env.at[0], left_f, local_sem.at[1])
    load_right = pltpu.make_async_copy(right_env.at[0, pl.ds(HALO, own_n)], right_f, local_sem.at[2])
    load_site.start()
    load_left.start()
    load_right.start()

    barrier = pltpu.get_barrier_semaphore()
    for step in (1, -1, 2, -2):
        pl.semaphore_signal(barrier, inc=1, device_id=other(step), device_id_type=MESH)
    pl.semaphore_wait(barrier, 4)

    def env_piece(i, side):
        at = pl.ds(side * half, half)
        return remote(
            right_env.at[0, W_DN * (1 - odd) + i, :, at], cross_f.at[i, :, at], cross_sem.at[side, i], cross
        )

    load_site.wait()
    move_site = remote(site_v.at[1], low_v, site_sem, other(1))
    move_site.start()
    for i in range(W_DN):
        env_piece(i, 0).start()
    move_near = remote(right_env.at[0, pl.ds(W_DN * odd, W_DN)], near_f, near_sem, near)
    move_near.start()

    rounds = []
    reach = 1
    while 2 * reach <= chips // 2:
        rounds.append(reach)
        reach *= 2

    def greet(i):
        if i < len(rounds):
            for step in (2 * rounds[i], -2 * rounds[i]):
                pl.semaphore_signal(known_sem.at[i], inc=1, device_id=other(step), device_id_type=MESH)

    def greeted(i):
        if i < len(rounds):
            pl.semaphore_wait(known_sem.at[i], 2)

    greet(0)

    own_size = sizes[me]
    low_size = jnp.where(me == 0, 0, sizes[lax.rem(me + n - 1, n)])

    def mask_pair(r0, rows, c0, c1=size, row_size=None):
        shape = (rows, c1 - c0)
        row = lax.broadcasted_iota(jnp.int32, shape, 0) + r0
        lane = lax.broadcasted_iota(jnp.int32, shape, 1) + c0
        return (row < (own_size if row_size is None else row_size)) & (lane < own_size)

    ortho_v[0] = jnp.where(mask_pair(0, size, 0), site_v[0], 0.0)
    row = lax.broadcasted_iota(jnp.int32, (size, size), 0)
    lane = lax.broadcasted_iota(jnp.int32, (size, size), 1)
    dead = ((row == lane) & (row >= own_size)).astype(f32)
    gram[...] = dot(ortho_v[0], ortho_v[0], ((0,), (0,)), precision=highest) + dead

    def split_right(source, offset):
        def body(i, _):
            at = pl.ds(pl.multiple_of((i + offset) * size, size), size)
            right_h[at, :], right_l[at, :] = split(source[i])
            return 0

        lax.fori_loop(0, source.shape[0], body, 0)

    load_left.wait()

    def split_left(count, source, target):
        def body(i, _):
            left_h[i + target], left_l[i + target] = split(left_f[i + source])
            return 0

        lax.fori_loop(0, count, body, 0)

    split_left(own_n, HALO, 0)
    split_left(W_DN, W_DN * (1 - odd), own_n)
    split_left(W_DN, W_DN * odd, met_n)
    load_right.wait()
    split_right(right_f, 0)
    greeted(0)
    greet(1)

    move_site.wait_recv()
    ortho_v[1] = jnp.where(mask_pair(0, size, 0, size, low_size), low_v[...], 0.0)
    gram[...] = gram[...] + dot(ortho_v[1], ortho_v[1], ((0,), (0,)), precision=highest)
    greeted(1)
    greet(2)

    sends = []

    def bond_piece(k, r0, c0):
        at = (pl.ds(r0, BLK), pl.ds(c0, size - c0))
        for side, (target, halo) in enumerate(((near, halo_n), (cross, halo_c))):
            copy = remote(bond.at[at], halo.at[at], bond_sem.at[side, k], target)
            copy.start()
            sends.append(copy)
        if k == 0:
            env_piece(0, 1).start()
            env_piece(1, 1).start()
        if k == size // BLK - 1:
            env_piece(2, 1).start()
            env_piece(3, 1).start()
            greeted(2)
            greet(3)

    bond[half:, :half] = jnp.zeros((half, half), f32)
    factorize(gram, upper, bond, inv, mask_pair, bond_piece)

    def stage_one(first, last, block):
        high, low = split(block)
        for a in range(first, last):
            at = slice(a * size, (a + 1) * size)
            mix_h[:, at], mix_l[:, at] = split(dot3(left_h[a], left_l[a], high, low))

    def stage_two(first, last, c0=0, c1=size):
        at = slice(first * size, last * size)
        return dot3(mix_h[:, at], mix_l[:, at], right_h[at, c0:c1], right_l[at, c0:c1])

    def bond_halo(ref):
        low = jnp.concatenate([jnp.zeros((half, half), f32), ref[half:, half:]], axis=1)
        return jnp.concatenate([ref[:half, :], low], axis=0)

    at_end = jnp.broadcast_to(lax.rem(me + 1, n), (size, size)) < 2
    has_cross = jnp.logical_not(at_end)

    stage_one(0, own_n, bond[...])
    move_near.wait_recv()
    split_right(near_f, own_n)
    for copy in sends[0::2]:
        copy.wait_recv()
    stage_one(own_n, met_n, bond_halo(halo_n))
    part_v[...] = stage_two(0, met_n)

    def ortho_rows(part):
        blocks = []
        for k in range(size // BLK):
            r0 = k * BLK
            c0 = r0 // 128 * 128
            want = ortho_v[part][:, c0 : c0 + 128]
            if k:
                done = jnp.concatenate(blocks, axis=1)
                want = want - dot(done, upper[:r0, c0 : c0 + 128], precision=highest)
            first = r0 - c0
            blocks.append(dot(want[:, first : first + BLK], inv[k][:, :BLK], ((1,), (1,)), precision=highest))
        return jnp.concatenate(blocks, axis=1)

    result_v[1] = ortho_rows(1)
    move_low = remote(result_v.at[1], left_out.at[0, 1], low_sem, other(-1))
    move_low.start()

    for copy in sends[1::2]:
        copy.wait_recv()
    stage_one(met_n, width, jnp.where(has_cross, bond_halo(halo_c), 0.0))

    def split_cross(first, last, side):
        at = slice(side * half, (side + 1) * half)
        for i in range(first, last):
            env_piece(i, side).wait_recv()
            rows = slice((met_n + i) * size, (met_n + i + 1) * size)
            right_h[rows, at], right_l[rows, at] = split(cross_f[i, :, at])

    app_sends = []
    for side in range(2):
        c0, c1 = side * half, (side + 1) * half
        total = part_v[:, c0:c1]
        for i in (0, 2) if side else (0,):
            count = 2 if side else W_DN
            split_cross(i, i + count, side)
            total = total + stage_two(met_n + i, met_n + i + count, c0, c1)
        app[:, c0:c1] = jnp.where(mask_pair(0, size, c0, c1), TAU * total, 0.0)
        at = pl.ds(c0, half)
        for to, (target, halo) in enumerate(((cross, app_c), (near, app_n))):
            copy = remote(app.at[:, at], halo.at[:, at], app_sem.at[to, side], target)
            copy.start()
            app_sends.append(copy)

    def total_of(x):
        return jnp.sum(jnp.sum(x, axis=0, keepdims=True), axis=1, keepdims=True)

    stage_one(0, own_n, app[...])
    for copy in app_sends[1::2]:
        copy.wait_recv()
    stage_one(own_n, met_n, app_n[...])
    part_v[...] = stage_two(0, met_n)
    b, a = bond[...], app[...]
    pieces = [total_of(x) for x in (b * b, b * a, a * a)]
    for copy in app_sends[0::2]:
        copy.wait_recv()
    stage_one(met_n, width, jnp.where(has_cross, app_c[...], 0.0))
    second[...] = jnp.where(mask_pair(0, size, 0), (0.5 * TAU) * (part_v[...] + stage_two(met_n, width)), 0.0)
    h = second[...]
    pieces += [total_of(x) for x in (bond[...] * h, app[...] * h, h * h)]
    lane_1 = lax.broadcasted_iota(jnp.int32, (1, 128), 1)
    packed = jnp.zeros((1, 128), f32)
    for i, piece in enumerate(pieces):
        packed = jnp.where(lane_1 == i, piece, packed)
    mine[0] = packed
    greeted(3)
    for i in range(4, len(rounds)):
        greet(i)
        greeted(i)

    def far(d):
        return pltpu.make_async_remote_copy(
            src_ref=mine.at[0], dst_ref=slots.at[d - 1], send_sem=far_sem.at[0, d - 1], recv_sem=far_sem.at[1, d - 1],
            device_id={"row": lax.rem(me + 2 * d, n)}, device_id_type=MESH,
        )

    def send_far(i, _):
        d = chips // 2 + (i + 1) // 2 * (2 * (i % 2) - 1)
        far(d).start()
        return 0

    lax.fori_loop(0, chips - 1, send_far, 0)

    result_v[0] = ortho_rows(0)
    store_up = pltpu.make_async_copy(result_v.at[0], left_out.at[0, 0], out_sem.at[0])
    store_up.start()

    def take_far(i, _):
        far(i + 1).wait_recv()
        return 0

    lax.fori_loop(0, chips - 1, take_far, 0)
    mine[1] = mine[0] + jnp.sum(slots[...], axis=0)
    swap = remote(mine.at[1], partner, pair_sem, near)
    swap.start()
    swap.wait_recv()
    sums = mine[1] + partner[...]
    bb, ba, aa, bh, ah, hh = (jnp.broadcast_to(sums[:, i : i + 1], (1, size)) for i in range(6))
    step = ba / bb
    weight_b = 1.0 - step + 0.5 * step * step
    weight_a = 1.0 - step
    norm = (
        weight_b * weight_b * bb + 2.0 * weight_b * weight_a * ba + weight_a * weight_a * aa
        + 2.0 * weight_b * bh + 2.0 * weight_a * ah + hh
    )
    scale = jnp.sqrt(bb / norm)
    bond_out[0] = (weight_b * bond[...] + weight_a * app[...] + second[...]) * scale

    def sent_far(i, _):
        far(i + 1).wait_send()
        return 0

    lax.fori_loop(0, chips - 1, sent_far, 0)
    pieces = [env_piece(i, side) for i in range(W_DN) for side in range(2)]
    for copy in (move_site, move_near, *pieces, *sends, *app_sends, swap, move_low):
        copy.wait_send()
    move_low.wait_recv()
    store_up.wait()


def on_device(n, site_tensor, left_env, right_env, sector_size):
    size = site_tensor.shape[-1]
    width = left_env.shape[1]
    full = (size, size)
    hbm = pl.BlockSpec(memory_space=pltpu.HBM)
    chips = n // 2
    parts = size // BLK
    scratch = [
        pltpu.VMEM((2, *full), f32), pltpu.VMEM(full, f32), pltpu.VMEM((width, *full), f32),
        pltpu.VMEM((width - HALO, *full), f32), pltpu.VMEM((W_DN, *full), f32), pltpu.VMEM((W_UP, *full), f32),
        pltpu.VMEM((width, *full), bf16), pltpu.VMEM((width, *full), bf16),
        pltpu.VMEM((width * size, size), bf16), pltpu.VMEM((width * size, size), bf16),
        pltpu.VMEM(full, f32), pltpu.VMEM(full, f32), pltpu.VMEM(full, f32), pltpu.VMEM((parts, BLK, 128), f32),
        *[pltpu.VMEM(full, f32)] * 7,
        pltpu.VMEM((size, width * size), bf16), pltpu.VMEM((size, width * size), bf16),
        pltpu.VMEM((2, *full), f32), pltpu.VMEM((2, *full), f32),
        pltpu.VMEM((2, 1, 128), f32), pltpu.VMEM((chips - 1, 1, 128), f32), pltpu.VMEM((1, 128), f32),
        pltpu.SemaphoreType.DMA((3,)), pltpu.SemaphoreType.DMA((1,)), pltpu.SemaphoreType.DMA((2,)),
        pltpu.SemaphoreType.DMA((2,)), pltpu.SemaphoreType.DMA((2, W_DN, 2)),
        pltpu.SemaphoreType.DMA((2, parts, 2)), pltpu.SemaphoreType.DMA((2, 2, 2)),
        pltpu.SemaphoreType.DMA((2,)), pltpu.SemaphoreType.DMA((2, chips - 1)), pltpu.SemaphoreType.DMA((2,)),
        pltpu.SemaphoreType.REGULAR((max(1, chips.bit_length()),)),
    ]
    return pl.pallas_call(
        functools.partial(kernel, n),
        out_shape=(
            jax.ShapeDtypeStruct((1, 2, *full), f32),
            jax.ShapeDtypeStruct((1, *full), f32),
        ),
        in_specs=[pl.BlockSpec(memory_space=pltpu.SMEM), hbm, hbm, hbm],
        out_specs=(hbm, pl.BlockSpec(memory_space=pltpu.VMEM)),
        scratch_shapes=scratch,
        compiler_params=pltpu.CompilerParams(
            collective_id=0, has_side_effects=True, vmem_limit_bytes=60 * 1024 * 1024
        ),
    )(sector_size, site_tensor, left_env, right_env)


def solution(mesh):
    block = P(("real", "row"), None, None, None)
    return jax.shard_map(
        functools.partial(on_device, mesh.shape["row"]),
        mesh=mesh,
        in_specs=(block, block, block, P("real")),
        out_specs=(block, P(("real", "row"), None, None)),
        check_vma=False,
    )
```

```python
import functools

import jax
import jax.numpy as jnp
from jax import lax
from jax.experimental import pallas as pl
from jax.experimental.pallas import tpu as pltpu
from jax.sharding import PartitionSpec as P

MESH = pl.DeviceIdType.MESH
W_DN = 4
W_UP = 4
HALO = W_DN + W_UP
TAU = 0.15
BLK = 64
highest = lax.Precision.HIGHEST
f32 = jnp.float32
bf16 = jnp.bfloat16


def across_lanes(tile, lane):
    return jnp.broadcast_to(tile[:, lane : lane + 1], tile.shape)


def across_rows(tile, row):
    return jnp.broadcast_to(tile[row : row + 1, :], tile.shape)


def eliminate(tiles, first):
    sub = lax.broadcasted_iota(jnp.int32, (8, 128), 0)
    count = len(tiles)
    tiles = [list(tile) for tile in tiles]
    own = [across_lanes(tiles[0][0], first + j) for j in range(8)]
    for g in range(count):
        last = g + 1 == count
        ahead = [] if last else [across_lanes(tiles[g + 1][0], first + 8 * (g + 1) + j) for j in range(8)]
        cols = {v: [across_lanes(tiles[v][0], first + 8 * g + j) for j in range(8)] for v in range(g + 1, count)}
        pivots = None
        for j in range(8):
            pivot = across_rows(own[j], j)
            inverse = 1.0 / pivot
            pivots = pivot if pivots is None else jnp.where(sub == j, pivot, pivots)
            heads = {k: across_rows(own[k], j) * inverse for k in range(j + 1, 8)}
            below = jnp.where(sub > j, own[j], 0.0)
            for k in range(j + 1, 8):
                own[k] = own[k] - below * heads[k]
            rows = [across_rows(part, j) * inverse for part in tiles[g]]
            tiles[g] = [part - below * row for part, row in zip(tiles[g], rows)]
            for v in range(g + 1, count):
                factor = cols[v][j]
                for k in range(j + 1, 8):
                    cols[v][k] = cols[v][k] - factor * heads[k]
                tiles[v] = [part - factor * row for part, row in zip(tiles[v], rows)]
            if not last:
                factor = cols[g + 1][j]
                scaled = factor * inverse
                ahead = [col - factor * across_rows(scaled, k) for k, col in enumerate(ahead)]
        scale = lax.rsqrt(pivots)
        tiles[g] = [part * scale for part in tiles[g]]
        own = ahead
    return tiles


def dot(a, b, dims=((1,), (0,)), precision=None):
    return lax.dot_general(a, b, (dims, ((), ())), precision=precision, preferred_element_type=f32)


def split(x):
    high = x.astype(bf16)
    return high, (x - high.astype(f32)).astype(bf16)


def dot3(ah, al, bh, bl):
    return dot(ah, bh) + dot(ah, bl) + dot(al, bh)


def factorize(gram, upper, bond, diag_inverse, mask_pair, done):
    size = gram.shape[0]
    lane = lax.broadcasted_iota(jnp.int32, (8, 128), 1)
    sub = lax.broadcasted_iota(jnp.int32, (8, 128), 0)
    for k in range(size // BLK):
        r0 = k * BLK
        c0 = r0 // 128 * 128
        first = r0 - c0
        tiles = []
        for g in range(BLK // 8):
            at = slice(r0 + 8 * g, r0 + 8 * g + 8)
            unit = (lane == sub + 8 * g).astype(f32)
            parts = [gram[at, c : c + 128] for c in range(c0, size, 128)]
            if first:
                parts[0] = jnp.where(lane >= first, parts[0], unit)
            else:
                parts.append(unit)
            tiles.append(parts)
        tiles = eliminate(tiles, first)
        parts = [jnp.concatenate([tile[i] for tile in tiles], axis=0) for i in range(len(tiles[0]))]
        diag_inverse[k] = parts[0] if first else parts.pop()
        lane_b = lax.broadcasted_iota(jnp.int32, (BLK, 128), 1)
        row_b = lax.broadcasted_iota(jnp.int32, (BLK, 128), 0)
        parts[0] = jnp.where(lane_b - first >= row_b, parts[0], 0.0)
        panel = jnp.concatenate(parts, axis=1) if len(parts) > 1 else parts[0]
        if r0 + BLK < size:
            if not first:
                turned = jnp.transpose(parts[0])[BLK:, :]
                at = slice(r0 + BLK, r0 + 2 * BLK)
                gram[at, c0:] = gram[at, c0:] - dot(turned, panel, precision=highest)
            if len(parts) > 1:
                turned = jnp.transpose(parts[1])
                gram[c0 + 128 :, c0 + 128 :] = gram[c0 + 128 :, c0 + 128 :] - dot(turned, parts[1], precision=highest)
        upper[r0 : r0 + BLK, c0:] = panel
        bond[r0 : r0 + BLK, c0:] = jnp.where(mask_pair(r0, BLK, c0), panel, 0.0)
        done(k, r0, c0)


def kernel(
    n, sizes, site, left_env, right_env, left_out, bond_out,
    site_v, low_v, left_f, right_f, near_f, cross_f, left_h, left_l, right_h, right_l,
    gram, upper, bond, inv, halo_n, halo_c, app, app_n, app_c, second, part_v, mix_h, mix_l,
    ortho_v, result_v, mine, slots, partner,
    local_sem, out_sem, site_sem, near_sem, cross_sem, bond_sem, app_sem, low_sem, far_sem, pair_sem, known_sem,
):
    me = lax.axis_index("row")
    odd = lax.rem(me, 2)
    size = site.shape[-1]
    half = size // 2
    width = left_env.shape[1]
    own_n = width - HALO
    met_n = own_n + W_DN
    chips = n // 2

    def other(step):
        return {"row": lax.rem(me + step + n, n)}

    near, cross = other(1 - 2 * odd), other(2 * odd - 1)

    def remote(src, dst, sems, target):
        return pltpu.make_async_remote_copy(
            src_ref=src, dst_ref=dst, send_sem=sems.at[0], recv_sem=sems.at[1], device_id=target, device_id_type=MESH
        )

    load_site = pltpu.make_async_copy(site.at[0], site_v, local_sem.at[0])
    load_left = pltpu.make_async_copy(left_env.at[0], left_f, local_sem.at[1])
    load_right = pltpu.make_async_copy(right_env.at[0, pl.ds(HALO, own_n)], right_f, local_sem.at[2])
    load_site.start()
    load_left.start()
    load_right.start()

    barrier = pltpu.get_barrier_semaphore()
    for step in (1, -1, 2, -2):
        pl.semaphore_signal(barrier, inc=1, device_id=other(step), device_id_type=MESH)
    pl.semaphore_wait(barrier, 4)

    def env_piece(i, side):
        at = pl.ds(side * half, half)
        return remote(
            right_env.at[0, W_DN * (1 - odd) + i, :, at], cross_f.at[i, :, at], cross_sem.at[side, i], cross
        )

    load_site.wait()
    move_site = remote(site_v.at[1], low_v, site_sem, other(1))
    move_site.start()
    for i in range(W_DN):
        env_piece(i, 0).start()
    move_near = remote(right_env.at[0, pl.ds(W_DN * odd, W_DN)], near_f, near_sem, near)
    move_near.start()

    rounds = []
    reach = 1
    while 2 * reach <= chips // 2:
        rounds.append(reach)
        reach *= 2

    def greet(i):
        if i < len(rounds):
            for step in (2 * rounds[i], -2 * rounds[i]):
                pl.semaphore_signal(known_sem.at[i], inc=1, device_id=other(step), device_id_type=MESH)

    def greeted(i):
        if i < len(rounds):
            pl.semaphore_wait(known_sem.at[i], 2)

    greet(0)

    own_size = sizes[me]
    low_size = jnp.where(me == 0, 0, sizes[lax.rem(me + n - 1, n)])

    def mask_pair(r0, rows, c0, c1=size, row_size=None):
        shape = (rows, c1 - c0)
        row = lax.broadcasted_iota(jnp.int32, shape, 0) + r0
        lane = lax.broadcasted_iota(jnp.int32, shape, 1) + c0
        return (row < (own_size if row_size is None else row_size)) & (lane < own_size)

    ortho_v[0] = jnp.where(mask_pair(0, size, 0), site_v[0], 0.0)
    row = lax.broadcasted_iota(jnp.int32, (size, size), 0)
    lane = lax.broadcasted_iota(jnp.int32, (size, size), 1)
    dead = ((row == lane) & (row >= own_size)).astype(f32)
    gram[...] = dot(ortho_v[0], ortho_v[0], ((0,), (0,)), precision=highest) + dead

    def split_right(source, offset):
        def body(i, _):
            at = pl.ds(pl.multiple_of((i + offset) * size, size), size)
            right_h[at, :], right_l[at, :] = split(source[i])
            return 0

        lax.fori_loop(0, source.shape[0], body, 0)

    load_left.wait()

    def split_left(count, source, target):
        def body(i, _):
            left_h[i + target], left_l[i + target] = split(left_f[i + source])
            return 0

        lax.fori_loop(0, count, body, 0)

    split_left(own_n, HALO, 0)
    split_left(W_DN, W_DN * (1 - odd), own_n)
    split_left(W_DN, W_DN * odd, met_n)
    load_right.wait()
    split_right(right_f, 0)
    greeted(0)
    greet(1)

    move_site.wait_recv()
    ortho_v[1] = jnp.where(mask_pair(0, size, 0, size, low_size), low_v[...], 0.0)
    gram[...] = gram[...] + dot(ortho_v[1], ortho_v[1], ((0,), (0,)), precision=highest)
    greeted(1)
    greet(2)

    sends = []

    def bond_piece(k, r0, c0):
        at = (pl.ds(r0, BLK), pl.ds(c0, size - c0))
        for side, (target, halo) in enumerate(((near, halo_n), (cross, halo_c))):
            copy = remote(bond.at[at], halo.at[at], bond_sem.at[side, k], target)
            copy.start()
            sends.append(copy)
        if k == 0:
            env_piece(0, 1).start()
            env_piece(1, 1).start()
        if k == size // BLK - 1:
            env_piece(2, 1).start()
            env_piece(3, 1).start()
            greeted(2)
            greet(3)

    bond[half:, :half] = jnp.zeros((half, half), f32)
    factorize(gram, upper, bond, inv, mask_pair, bond_piece)

    def stage_one(first, last, block):
        high, low = split(block)
        for a in range(first, last):
            at = slice(a * size, (a + 1) * size)
            mix_h[:, at], mix_l[:, at] = split(dot3(left_h[a], left_l[a], high, low))

    def stage_two(first, last, c0=0, c1=size):
        at = slice(first * size, last * size)
        return dot3(mix_h[:, at], mix_l[:, at], right_h[at, c0:c1], right_l[at, c0:c1])

    def bond_halo(ref):
        low = jnp.concatenate([jnp.zeros((half, half), f32), ref[half:, half:]], axis=1)
        return jnp.concatenate([ref[:half, :], low], axis=0)

    at_end = jnp.broadcast_to(lax.rem(me + 1, n), (size, size)) < 2
    has_cross = jnp.logical_not(at_end)

    stage_one(0, own_n, bond[...])
    move_near.wait_recv()
    split_right(near_f, own_n)
    for copy in sends[0::2]:
        copy.wait_recv()
    stage_one(own_n, met_n, bond_halo(halo_n))
    part_v[...] = stage_two(0, met_n)

    def ortho_rows(part):
        blocks = []
        for k in range(size // BLK):
            r0 = k * BLK
            c0 = r0 // 128 * 128
            want = ortho_v[part][:, c0 : c0 + 128]
            if k:
                done = jnp.concatenate(blocks, axis=1)
                want = want - dot(done, upper[:r0, c0 : c0 + 128], precision=highest)
            first = r0 - c0
            blocks.append(dot(want[:, first : first + BLK], inv[k][:, :BLK], ((1,), (1,)), precision=highest))
        return jnp.concatenate(blocks, axis=1)

    result_v[1] = ortho_rows(1)
    move_low = remote(result_v.at[1], left_out.at[0, 1], low_sem, other(-1))
    move_low.start()

    for copy in sends[1::2]:
        copy.wait_recv()
    stage_one(met_n, width, jnp.where(has_cross, bond_halo(halo_c), 0.0))

    def split_cross(first, last, side):
        at = slice(side * half, (side + 1) * half)
        for i in range(first, last):
            env_piece(i, side).wait_recv()
            rows = slice((met_n + i) * size, (met_n + i + 1) * size)
            right_h[rows, at], right_l[rows, at] = split(cross_f[i, :, at])

    app_sends = []
    for side in range(2):
        c0, c1 = side * half, (side + 1) * half
        total = part_v[:, c0:c1]
        for i in (0, 2) if side else (0,):
            count = 2 if side else W_DN
            split_cross(i, i + count, side)
            total = total + stage_two(met_n + i, met_n + i + count, c0, c1)
        app[:, c0:c1] = jnp.where(mask_pair(0, size, c0, c1), TAU * total, 0.0)
        at = pl.ds(c0, half)
        for to, (target, halo) in enumerate(((cross, app_c), (near, app_n))):
            copy = remote(app.at[:, at], halo.at[:, at], app_sem.at[to, side], target)
            copy.start()
            app_sends.append(copy)

    def total_of(x):
        return jnp.sum(jnp.sum(x, axis=0, keepdims=True), axis=1, keepdims=True)

    stage_one(0, own_n, app[...])
    for copy in app_sends[1::2]:
        copy.wait_recv()
    stage_one(own_n, met_n, app_n[...])
    part_v[...] = stage_two(0, met_n)
    greeted(3)
    for i in range(4, len(rounds)):
        greet(i)
        greeted(i)
    pl.semaphore_signal(known_sem.at[len(rounds)], inc=1, device_id=near, device_id_type=MESH)
    b, a = bond[...], app[...]
    pieces = [total_of(x) for x in (b * b, b * a, a * a)]
    for copy in app_sends[0::2]:
        copy.wait_recv()
    stage_one(met_n, width, jnp.where(has_cross, app_c[...], 0.0))
    second[...] = jnp.where(mask_pair(0, size, 0), (0.5 * TAU) * (part_v[...] + stage_two(met_n, width)), 0.0)
    h = second[...]
    pieces += [total_of(x) for x in (bond[...] * h, app[...] * h, h * h)]
    lane_1 = lax.broadcasted_iota(jnp.int32, (1, 128), 1)
    packed = jnp.zeros((1, 128), f32)
    for i, piece in enumerate(pieces):
        packed = jnp.where(lane_1 == i, piece, packed)
    mine[...] = packed
    pl.semaphore_wait(known_sem.at[len(rounds)], 1)

    def far(d, core):
        slot = (chips - 1) * core + d - 1
        return pltpu.make_async_remote_copy(
            src_ref=mine, dst_ref=slots.at[slot], send_sem=far_sem.at[0, slot], recv_sem=far_sem.at[1, slot],
            device_id={"row": lax.rem(me + 2 * d, n) + core * (1 - 2 * odd)}, device_id_type=MESH,
        )

    swap = remote(mine, partner, pair_sem, near)

    def send_far(i, _):
        d = chips // 2 + (i + 1) // 2 * (2 * (i % 2) - 1)
        far(d, 0).start()
        far(d, 1).start()
        return 0

    lax.fori_loop(0, chips - 1, send_far, 0)
    swap.start()

    result_v[0] = ortho_rows(0)
    store_up = pltpu.make_async_copy(result_v.at[0], left_out.at[0, 0], out_sem.at[0])
    store_up.start()

    def take_far(i, _):
        far(i + 1, 0).wait_recv()
        far(i + 1, 1).wait_recv()
        return 0

    lax.fori_loop(0, chips - 1, take_far, 0)
    swap.wait_recv()
    sums = mine[...] + partner[...] + jnp.sum(slots[...], axis=0)
    bb, ba, aa, bh, ah, hh = (jnp.broadcast_to(sums[:, i : i + 1], (1, size)) for i in range(6))
    step = ba / bb
    weight_b = 1.0 - step + 0.5 * step * step
    weight_a = 1.0 - step
    norm = (
        weight_b * weight_b * bb + 2.0 * weight_b * weight_a * ba + weight_a * weight_a * aa
        + 2.0 * weight_b * bh + 2.0 * weight_a * ah + hh
    )
    scale = jnp.sqrt(bb / norm)
    bond_out[0] = (weight_b * bond[...] + weight_a * app[...] + second[...]) * scale

    def sent_far(i, _):
        far(i + 1, 0).wait_send()
        far(i + 1, 1).wait_send()
        return 0

    lax.fori_loop(0, chips - 1, sent_far, 0)
    pieces = [env_piece(i, side) for i in range(W_DN) for side in range(2)]
    for copy in (move_site, move_near, *pieces, *sends, *app_sends, swap, move_low):
        copy.wait_send()
    move_low.wait_recv()
    store_up.wait()


def on_device(n, site_tensor, left_env, right_env, sector_size):
    size = site_tensor.shape[-1]
    width = left_env.shape[1]
    full = (size, size)
    hbm = pl.BlockSpec(memory_space=pltpu.HBM)
    chips = n // 2
    parts = size // BLK
    scratch = [
        pltpu.VMEM((2, *full), f32), pltpu.VMEM(full, f32), pltpu.VMEM((width, *full), f32),
        pltpu.VMEM((width - HALO, *full), f32), pltpu.VMEM((W_DN, *full), f32), pltpu.VMEM((W_UP, *full), f32),
        pltpu.VMEM((width, *full), bf16), pltpu.VMEM((width, *full), bf16),
        pltpu.VMEM((width * size, size), bf16), pltpu.VMEM((width * size, size), bf16),
        pltpu.VMEM(full, f32), pltpu.VMEM(full, f32), pltpu.VMEM(full, f32), pltpu.VMEM((parts, BLK, 128), f32),
        *[pltpu.VMEM(full, f32)] * 7,
        pltpu.VMEM((size, width * size), bf16), pltpu.VMEM((size, width * size), bf16),
        pltpu.VMEM((2, *full), f32), pltpu.VMEM((2, *full), f32),
        pltpu.VMEM((1, 128), f32), pltpu.VMEM((2 * chips - 2, 1, 128), f32), pltpu.VMEM((1, 128), f32),
        pltpu.SemaphoreType.DMA((3,)), pltpu.SemaphoreType.DMA((1,)), pltpu.SemaphoreType.DMA((2,)),
        pltpu.SemaphoreType.DMA((2,)), pltpu.SemaphoreType.DMA((2, W_DN, 2)),
        pltpu.SemaphoreType.DMA((2, parts, 2)), pltpu.SemaphoreType.DMA((2, 2, 2)),
        pltpu.SemaphoreType.DMA((2,)), pltpu.SemaphoreType.DMA((2, 2 * chips - 2)), pltpu.SemaphoreType.DMA((2,)),
        pltpu.SemaphoreType.REGULAR((max(1, chips.bit_length()),)),
    ]
    return pl.pallas_call(
        functools.partial(kernel, n),
        out_shape=(
            jax.ShapeDtypeStruct((1, 2, *full), f32),
            jax.ShapeDtypeStruct((1, *full), f32),
        ),
        in_specs=[pl.BlockSpec(memory_space=pltpu.SMEM), hbm, hbm, hbm],
        out_specs=(hbm, pl.BlockSpec(memory_space=pltpu.VMEM)),
        scratch_shapes=scratch,
        compiler_params=pltpu.CompilerParams(
            collective_id=0, has_side_effects=True, vmem_limit_bytes=53 * 1024 * 1024
        ),
    )(sector_size, site_tensor, left_env, right_env)


def solution(mesh):
    block = P(("real", "row"), None, None, None)
    return jax.shard_map(
        functools.partial(on_device, mesh.shape["row"]),
        mesh=mesh,
        in_specs=(block, block, block, P("real")),
        out_specs=(block, P(("real", "row"), None, None)),
        check_vma=False,
    )
```

```python
import functools

import jax
import jax.numpy as jnp
from jax import lax
from jax.experimental import pallas as pl
from jax.experimental.pallas import tpu as pltpu
from jax.sharding import PartitionSpec as P

MESH = pl.DeviceIdType.MESH
W_DN = 4
W_UP = 4
HALO = W_DN + W_UP
TAU = 0.15
BLK = 64
highest = lax.Precision.HIGHEST
f32 = jnp.float32
bf16 = jnp.bfloat16


def across_lanes(tile, lane):
    return jnp.broadcast_to(tile[:, lane : lane + 1], tile.shape)


def across_rows(tile, row):
    return jnp.broadcast_to(tile[row : row + 1, :], tile.shape)


def eliminate(tiles, first):
    sub = lax.broadcasted_iota(jnp.int32, (8, 128), 0)
    count = len(tiles)
    tiles = [list(tile) for tile in tiles]
    own = [across_lanes(tiles[0][0], first + j) for j in range(8)]
    for g in range(count):
        last = g + 1 == count
        ahead = [] if last else [across_lanes(tiles[g + 1][0], first + 8 * (g + 1) + j) for j in range(8)]
        cols = {v: [across_lanes(tiles[v][0], first + 8 * g + j) for j in range(8)] for v in range(g + 1, count)}
        pivots = None
        for j in range(8):
            pivot = across_rows(own[j], j)
            inverse = 1.0 / pivot
            pivots = pivot if pivots is None else jnp.where(sub == j, pivot, pivots)
            heads = {k: across_rows(own[k], j) * inverse for k in range(j + 1, 8)}
            below = jnp.where(sub > j, own[j], 0.0)
            for k in range(j + 1, 8):
                own[k] = own[k] - below * heads[k]
            rows = [across_rows(part, j) * inverse for part in tiles[g]]
            tiles[g] = [part - below * row for part, row in zip(tiles[g], rows)]
            for v in range(g + 1, count):
                factor = cols[v][j]
                for k in range(j + 1, 8):
                    cols[v][k] = cols[v][k] - factor * heads[k]
                tiles[v] = [part - factor * row for part, row in zip(tiles[v], rows)]
            if not last:
                factor = cols[g + 1][j]
                scaled = factor * inverse
                ahead = [col - factor * across_rows(scaled, k) for k, col in enumerate(ahead)]
        scale = lax.rsqrt(pivots)
        tiles[g] = [part * scale for part in tiles[g]]
        own = ahead
    return tiles


def dot(a, b, dims=((1,), (0,)), precision=None):
    return lax.dot_general(a, b, (dims, ((), ())), precision=precision, preferred_element_type=f32)


def split(x):
    high = x.astype(bf16)
    return high, (x - high.astype(f32)).astype(bf16)


def dot3(ah, al, bh, bl):
    return dot(ah, bh) + dot(ah, bl) + dot(al, bh)


def factorize(gram, upper, bond, diag_inverse, mask_pair, done):
    size = gram.shape[0]
    lane = lax.broadcasted_iota(jnp.int32, (8, 128), 1)
    sub = lax.broadcasted_iota(jnp.int32, (8, 128), 0)
    for k in range(size // BLK):
        r0 = k * BLK
        c0 = r0 // 128 * 128
        first = r0 - c0
        tiles = []
        for g in range(BLK // 8):
            at = slice(r0 + 8 * g, r0 + 8 * g + 8)
            unit = (lane == sub + 8 * g).astype(f32)
            parts = [gram[at, c : c + 128] for c in range(c0, size, 128)]
            if first:
                parts[0] = jnp.where(lane >= first, parts[0], unit)
            else:
                parts.append(unit)
            tiles.append(parts)
        tiles = eliminate(tiles, first)
        parts = [jnp.concatenate([tile[i] for tile in tiles], axis=0) for i in range(len(tiles[0]))]
        diag_inverse[k] = parts[0] if first else parts.pop()
        lane_b = lax.broadcasted_iota(jnp.int32, (BLK, 128), 1)
        row_b = lax.broadcasted_iota(jnp.int32, (BLK, 128), 0)
        parts[0] = jnp.where(lane_b - first >= row_b, parts[0], 0.0)
        panel = jnp.concatenate(parts, axis=1) if len(parts) > 1 else parts[0]
        if r0 + BLK < size:
            if not first:
                turned = jnp.transpose(parts[0])[BLK:, :]
                at = slice(r0 + BLK, r0 + 2 * BLK)
                gram[at, c0:] = gram[at, c0:] - dot(turned, panel, precision=highest)
            if len(parts) > 1:
                turned = jnp.transpose(parts[1])
                gram[c0 + 128 :, c0 + 128 :] = gram[c0 + 128 :, c0 + 128 :] - dot(turned, parts[1], precision=highest)
        upper[r0 : r0 + BLK, c0:] = panel
        bond[r0 : r0 + BLK, c0:] = jnp.where(mask_pair(r0, BLK, c0), panel, 0.0)
        done(k, r0, c0)


def kernel(
    n, size_list, site, left_env, right_env, left_out, bond_out,
    sizes,    site_v, low_v, left_f, right_f, near_f, cross_f, left_h, left_l, right_h, right_l,
    gram, upper, bond, inv, halo_n, halo_c, app, app_n, app_c, second, part_v, mix_h, mix_l,
    ortho_v, result_v, mine, slots, partner,
    local_sem, out_sem, site_sem, near_sem, cross_sem, bond_sem, app_sem, low_sem, far_sem, pair_sem, known_sem,
):
    me = lax.axis_index("row")
    odd = lax.rem(me, 2)
    size = site.shape[-1]
    half = size // 2
    width = left_env.shape[1]
    own_n = width - HALO
    met_n = own_n + W_DN
    chips = n // 2

    def other(step):
        return {"row": lax.rem(me + step + n, n)}

    near, cross = other(1 - 2 * odd), other(2 * odd - 1)

    def remote(src, dst, sems, target):
        return pltpu.make_async_remote_copy(
            src_ref=src, dst_ref=dst, send_sem=sems.at[0], recv_sem=sems.at[1], device_id=target, device_id_type=MESH
        )

    load_site = pltpu.make_async_copy(site.at[0], site_v, local_sem.at[0])
    load_left = pltpu.make_async_copy(left_env.at[0], left_f, local_sem.at[1])
    load_right = pltpu.make_async_copy(right_env.at[0, pl.ds(HALO, own_n)], right_f, local_sem.at[2])
    load_sizes = pltpu.make_async_copy(size_list, sizes, local_sem.at[3])
    load_site.start()
    load_sizes.start()
    load_left.start()
    load_right.start()

    barrier = pltpu.get_barrier_semaphore()
    for step in (1, -1, 2, -2):
        pl.semaphore_signal(barrier, inc=1, device_id=other(step), device_id_type=MESH)
    pl.semaphore_wait(barrier, 4)

    def env_piece(i, side):
        at = pl.ds(side * half, half)
        return remote(
            right_env.at[0, W_DN * (1 - odd) + i, :, at], cross_f.at[i, :, at], cross_sem.at[side, i], cross
        )

    load_site.wait()
    move_site = remote(site_v.at[1], low_v, site_sem, other(1))
    move_site.start()
    for i in range(W_DN):
        env_piece(i, 0).start()
    move_near = remote(right_env.at[0, pl.ds(W_DN * odd, W_DN)], near_f, near_sem, near)
    move_near.start()

    rounds = []
    reach = 1
    while 2 * reach <= chips // 2:
        rounds.append(reach)
        reach *= 2

    def greet(i):
        if i < len(rounds):
            for step in (2 * rounds[i], -2 * rounds[i]):
                pl.semaphore_signal(known_sem.at[i], inc=1, device_id=other(step), device_id_type=MESH)

    def greeted(i):
        if i < len(rounds):
            pl.semaphore_wait(known_sem.at[i], 2)

    greet(0)

    load_sizes.wait()
    own_size = sizes[me]
    low_size = jnp.where(me == 0, 0, sizes[lax.rem(me + n - 1, n)])

    def mask_pair(r0, rows, c0, c1=size, row_size=None):
        shape = (rows, c1 - c0)
        row = lax.broadcasted_iota(jnp.int32, shape, 0) + r0
        lane = lax.broadcasted_iota(jnp.int32, shape, 1) + c0
        return (row < (own_size if row_size is None else row_size)) & (lane < own_size)

    ortho_v[0] = jnp.where(mask_pair(0, size, 0), site_v[0], 0.0)
    row = lax.broadcasted_iota(jnp.int32, (size, size), 0)
    lane = lax.broadcasted_iota(jnp.int32, (size, size), 1)
    dead = ((row == lane) & (row >= own_size)).astype(f32)
    gram[...] = dot(ortho_v[0], ortho_v[0], ((0,), (0,)), precision=highest) + dead

    def split_right(source, offset):
        def body(i, _):
            at = pl.ds(pl.multiple_of((i + offset) * size, size), size)
            right_h[at, :], right_l[at, :] = split(source[i])
            return 0

        lax.fori_loop(0, source.shape[0], body, 0)

    load_left.wait()

    def split_left(count, source, target):
        def body(i, _):
            left_h[i + target], left_l[i + target] = split(left_f[i + source])
            return 0

        lax.fori_loop(0, count, body, 0)

    split_left(own_n, HALO, 0)
    split_left(W_DN, W_DN * (1 - odd), own_n)
    split_left(W_DN, W_DN * odd, met_n)
    load_right.wait()
    split_right(right_f, 0)
    greeted(0)
    greet(1)

    move_site.wait_recv()
    ortho_v[1] = jnp.where(mask_pair(0, size, 0, size, low_size), low_v[...], 0.0)
    gram[...] = gram[...] + dot(ortho_v[1], ortho_v[1], ((0,), (0,)), precision=highest)
    greeted(1)
    greet(2)

    sends = []

    def bond_piece(k, r0, c0):
        at = (pl.ds(r0, BLK), pl.ds(c0, size - c0))
        for side, (target, halo) in enumerate(((near, halo_n), (cross, halo_c))):
            copy = remote(bond.at[at], halo.at[at], bond_sem.at[side, k], target)
            copy.start()
            sends.append(copy)
        if k == 0:
            env_piece(0, 1).start()
            env_piece(1, 1).start()
        if k == size // BLK - 1:
            env_piece(2, 1).start()
            env_piece(3, 1).start()
            greeted(2)
            greet(3)

    bond[half:, :half] = jnp.zeros((half, half), f32)
    factorize(gram, upper, bond, inv, mask_pair, bond_piece)

    def stage_one(first, last, block):
        high, low = split(block)
        for a in range(first, last):
            at = slice(a * size, (a + 1) * size)
            mix_h[:, at], mix_l[:, at] = split(dot3(left_h[a], left_l[a], high, low))

    def stage_two(first, last, c0=0, c1=size):
        at = slice(first * size, last * size)
        return dot3(mix_h[:, at], mix_l[:, at], right_h[at, c0:c1], right_l[at, c0:c1])

    def bond_halo(ref):
        low = jnp.concatenate([jnp.zeros((half, half), f32), ref[half:, half:]], axis=1)
        return jnp.concatenate([ref[:half, :], low], axis=0)

    at_end = jnp.broadcast_to(lax.rem(me + 1, n), (size, size)) < 2
    has_cross = jnp.logical_not(at_end)

    stage_one(0, own_n, bond[...])
    move_near.wait_recv()
    split_right(near_f, own_n)
    for copy in sends[0::2]:
        copy.wait_recv()
    stage_one(own_n, met_n, bond_halo(halo_n))
    part_v[...] = stage_two(0, met_n)

    def ortho_columns(part, blocks):
        for k in blocks:
            r0 = k * BLK
            c0 = r0 // 128 * 128
            want = ortho_v[part, :, c0 : c0 + 128]
            if k:
                want = want - dot(result_v[part, :, :r0], upper[:r0, c0 : c0 + 128], precision=highest)
            first = r0 - c0
            want = want[:, first : first + BLK]
            result_v[part, :, r0 : r0 + BLK] = dot(want, inv[k][:, :BLK], ((1,), (1,)), precision=highest)

    for copy in sends[1::2]:
        copy.wait_recv()
    stage_one(met_n, width, jnp.where(has_cross, bond_halo(halo_c), 0.0))

    def split_cross(first, last, side):
        at = slice(side * half, (side + 1) * half)
        for i in range(first, last):
            env_piece(i, side).wait_recv()
            rows = slice((met_n + i) * size, (met_n + i + 1) * size)
            right_h[rows, at], right_l[rows, at] = split(cross_f[i, :, at])

    app_sends = []
    for side in range(2):
        c0, c1 = side * half, (side + 1) * half
        total = part_v[:, c0:c1]
        for i in (0, 2) if side else (0,):
            count = 2 if side else W_DN
            split_cross(i, i + count, side)
            total = total + stage_two(met_n + i, met_n + i + count, c0, c1)
        app[:, c0:c1] = jnp.where(mask_pair(0, size, c0, c1), TAU * total, 0.0)
        at = pl.ds(c0, half)
        for to, (target, halo) in enumerate(((cross, app_c), (near, app_n))):
            copy = remote(app.at[:, at], halo.at[:, at], app_sem.at[to, side], target)
            copy.start()
            app_sends.append(copy)
        if side == 0:
            ortho_columns(1, range(size // BLK // 2))

    def total_of(x):
        return jnp.sum(jnp.sum(x, axis=0, keepdims=True), axis=1, keepdims=True)

    stage_one(0, own_n, app[...])
    for copy in app_sends[1::2]:
        copy.wait_recv()
    stage_one(own_n, met_n, app_n[...])
    part_v[...] = stage_two(0, met_n)
    greeted(3)
    for i in range(4, len(rounds)):
        greet(i)
        greeted(i)
    pl.semaphore_signal(known_sem.at[len(rounds)], inc=1, device_id=near, device_id_type=MESH)
    ortho_columns(1, range(size // BLK // 2, size // BLK))
    move_low = remote(result_v.at[1], left_out.at[0, 1], low_sem, other(-1))
    move_low.start()
    b, a = bond[...], app[...]
    pieces = [total_of(x) for x in (b * b, b * a, a * a)]
    for copy in app_sends[0::2]:
        copy.wait_recv()
    stage_one(met_n, width, jnp.where(has_cross, app_c[...], 0.0))
    second[...] = jnp.where(mask_pair(0, size, 0), (0.5 * TAU) * (part_v[...] + stage_two(met_n, width)), 0.0)
    h = second[...]
    pieces += [total_of(x) for x in (bond[...] * h, app[...] * h, h * h)]
    lane_1 = lax.broadcasted_iota(jnp.int32, (1, 128), 1)
    packed = jnp.zeros((1, 128), f32)
    for i, piece in enumerate(pieces):
        packed = jnp.where(lane_1 == i, piece, packed)
    mine[...] = packed
    pl.semaphore_wait(known_sem.at[len(rounds)], 1)

    def far(d, core):
        slot = (chips - 1) * core + d - 1
        return pltpu.make_async_remote_copy(
            src_ref=mine, dst_ref=slots.at[slot], send_sem=far_sem.at[0, slot], recv_sem=far_sem.at[1, slot],
            device_id={"row": lax.rem(me + 2 * d, n) + core * (1 - 2 * odd)}, device_id_type=MESH,
        )

    swap = remote(mine, partner, pair_sem, near)

    def send_far(i, _):
        d = chips // 2 + (i + 1) // 2 * (2 * (i % 2) - 1)
        far(d, 0).start()
        far(d, 1).start()
        return 0

    lax.fori_loop(0, chips - 1, send_far, 0)
    swap.start()

    ortho_columns(0, range(size // BLK))
    store_up = pltpu.make_async_copy(result_v.at[0], left_out.at[0, 0], out_sem.at[0])
    store_up.start()

    def take_far(i, _):
        far(i + 1, 0).wait_recv()
        far(i + 1, 1).wait_recv()
        return 0

    lax.fori_loop(0, chips - 1, take_far, 0)
    swap.wait_recv()
    sums = mine[...] + partner[...] + jnp.sum(slots[...], axis=0)
    bb, ba, aa, bh, ah, hh = (jnp.broadcast_to(sums[:, i : i + 1], (1, size)) for i in range(6))
    step = ba / bb
    weight_b = 1.0 - step + 0.5 * step * step
    weight_a = 1.0 - step
    norm = (
        weight_b * weight_b * bb + 2.0 * weight_b * weight_a * ba + weight_a * weight_a * aa
        + 2.0 * weight_b * bh + 2.0 * weight_a * ah + hh
    )
    scale = jnp.sqrt(bb / norm)
    bond_out[0] = (weight_b * bond[...] + weight_a * app[...] + second[...]) * scale

    def sent_far(i, _):
        far(i + 1, 0).wait_send()
        far(i + 1, 1).wait_send()
        return 0

    lax.fori_loop(0, chips - 1, sent_far, 0)
    pieces = [env_piece(i, side) for i in range(W_DN) for side in range(2)]
    for copy in (move_site, move_near, *pieces, *sends, *app_sends, swap, move_low):
        copy.wait_send()
    move_low.wait_recv()
    store_up.wait()


def store(left, bond, left_out, bond_out, sems):
    copies = [
        pltpu.make_async_copy(left, left_out, sems.at[0]),
        pltpu.make_async_copy(bond, bond_out, sems.at[1]),
    ]
    for copy in copies:
        copy.start()
    for copy in copies:
        copy.wait()


def stored(left, bond):
    here = pl.BlockSpec(memory_space=pltpu.VMEM)
    out = pl.BlockSpec(memory_space=pltpu.HBM)
    return pl.pallas_call(
        store,
        out_shape=(jax.ShapeDtypeStruct(left.shape, f32), jax.ShapeDtypeStruct(bond.shape, f32)),
        in_specs=[here, here],
        out_specs=(out, out),
        scratch_shapes=[pltpu.SemaphoreType.DMA((2,))],
        compiler_params=pltpu.CompilerParams(vmem_limit_bytes=4 * 1024 * 1024),
    )(left, bond)


def on_device(n, site_tensor, left_env, right_env, sector_size):
    size = site_tensor.shape[-1]
    width = left_env.shape[1]
    full = (size, size)
    hbm = pl.BlockSpec(memory_space=pltpu.HBM)
    chips = n // 2
    parts = size // BLK
    scratch = [
        pltpu.SMEM(sector_size.shape, jnp.int32), pltpu.VMEM((2, *full), f32), pltpu.VMEM(full, f32), pltpu.VMEM((width, *full), f32),
        pltpu.VMEM((width - HALO, *full), f32), pltpu.VMEM((W_DN, *full), f32), pltpu.VMEM((W_UP, *full), f32),
        pltpu.VMEM((width, *full), bf16), pltpu.VMEM((width, *full), bf16),
        pltpu.VMEM((width * size, size), bf16), pltpu.VMEM((width * size, size), bf16),
        pltpu.VMEM(full, f32), pltpu.VMEM(full, f32), pltpu.VMEM(full, f32), pltpu.VMEM((parts, BLK, 128), f32),
        *[pltpu.VMEM(full, f32)] * 7,
        pltpu.VMEM((size, width * size), bf16), pltpu.VMEM((size, width * size), bf16),
        pltpu.VMEM((2, *full), f32), pltpu.VMEM((2, *full), f32),
        pltpu.VMEM((1, 128), f32), pltpu.VMEM((2 * chips - 2, 1, 128), f32), pltpu.VMEM((1, 128), f32),
        pltpu.SemaphoreType.DMA((4,)), pltpu.SemaphoreType.DMA((1,)), pltpu.SemaphoreType.DMA((2,)),
        pltpu.SemaphoreType.DMA((2,)), pltpu.SemaphoreType.DMA((2, W_DN, 2)),
        pltpu.SemaphoreType.DMA((2, parts, 2)), pltpu.SemaphoreType.DMA((2, 2, 2)),
        pltpu.SemaphoreType.DMA((2,)), pltpu.SemaphoreType.DMA((2, 2 * chips - 2)), pltpu.SemaphoreType.DMA((2,)),
        pltpu.SemaphoreType.REGULAR((max(1, chips.bit_length()),)),
    ]
    left, bond = pl.pallas_call(
        functools.partial(kernel, n),
        out_shape=(
            jax.ShapeDtypeStruct((1, 2, *full), f32),
            jax.ShapeDtypeStruct((1, *full), f32),
        ),
        in_specs=[hbm, hbm, hbm, hbm],
        out_specs=(hbm, pl.BlockSpec(memory_space=pltpu.VMEM)),
        scratch_shapes=scratch,
        compiler_params=pltpu.CompilerParams(
            collective_id=0, has_side_effects=True, vmem_limit_bytes=53 * 1024 * 1024
        ),
    )(pltpu.with_memory_space_constraint(sector_size, pltpu.HBM), site_tensor, left_env, right_env)
    return stored(left, bond)


def solution(mesh):
    block = P(("real", "row"), None, None, None)
    return jax.shard_map(
        functools.partial(on_device, mesh.shape["row"]),
        mesh=mesh,
        in_specs=(block, block, block, P("real")),
        out_specs=(block, P(("real", "row"), None, None)),
        check_vma=False,
    )
```

```python
import functools

import jax
import jax.numpy as jnp
from jax import lax
from jax.experimental import pallas as pl
from jax.experimental.pallas import tpu as pltpu
from jax.sharding import PartitionSpec as P

MESH = pl.DeviceIdType.MESH
W_DN = 4
W_UP = 4
HALO = W_DN + W_UP
TAU = 0.15
BLK = 64
highest = lax.Precision.HIGHEST
f32 = jnp.float32
bf16 = jnp.bfloat16


def across_lanes(tile, lane):
    return jnp.broadcast_to(tile[:, lane : lane + 1], tile.shape)


def across_rows(tile, row):
    return jnp.broadcast_to(tile[row : row + 1, :], tile.shape)


def eliminate(tiles, first):
    sub = lax.broadcasted_iota(jnp.int32, (8, 128), 0)
    count = len(tiles)
    tiles = [list(tile) for tile in tiles]
    own = [across_lanes(tiles[0][0], first + j) for j in range(8)]
    for g in range(count):
        last = g + 1 == count
        ahead = [] if last else [across_lanes(tiles[g + 1][0], first + 8 * (g + 1) + j) for j in range(8)]
        cols = {v: [across_lanes(tiles[v][0], first + 8 * g + j) for j in range(8)] for v in range(g + 1, count)}
        pivots = None
        for j in range(8):
            pivot = across_rows(own[j], j)
            inverse = 1.0 / pivot
            pivots = pivot if pivots is None else jnp.where(sub == j, pivot, pivots)
            heads = {k: across_rows(own[k], j) * inverse for k in range(j + 1, 8)}
            below = jnp.where(sub > j, own[j], 0.0)
            for k in range(j + 1, 8):
                own[k] = own[k] - below * heads[k]
            rows = [across_rows(part, j) * inverse for part in tiles[g]]
            tiles[g] = [part - below * row for part, row in zip(tiles[g], rows)]
            for v in range(g + 1, count):
                factor = cols[v][j]
                for k in range(j + 1, 8):
                    cols[v][k] = cols[v][k] - factor * heads[k]
                tiles[v] = [part - factor * row for part, row in zip(tiles[v], rows)]
            if not last:
                factor = cols[g + 1][j]
                scaled = factor * inverse
                ahead = [col - factor * across_rows(scaled, k) for k, col in enumerate(ahead)]
        scale = lax.rsqrt(pivots)
        tiles[g] = [part * scale for part in tiles[g]]
        own = ahead
    return tiles


def dot(a, b, dims=((1,), (0,)), precision=None):
    return lax.dot_general(a, b, (dims, ((), ())), precision=precision, preferred_element_type=f32)


def split(x):
    high = x.astype(bf16)
    return high, (x - high.astype(f32)).astype(bf16)


def dot3(ah, al, bh, bl):
    return dot(ah, bh) + dot(ah, bl) + dot(al, bh)


def factorize(gram, upper, bond, diag_inverse, mask_pair, done):
    size = gram.shape[0]
    lane = lax.broadcasted_iota(jnp.int32, (8, 128), 1)
    sub = lax.broadcasted_iota(jnp.int32, (8, 128), 0)
    for k in range(size // BLK):
        r0 = k * BLK
        c0 = r0 // 128 * 128
        first = r0 - c0
        tiles = []
        for g in range(BLK // 8):
            at = slice(r0 + 8 * g, r0 + 8 * g + 8)
            unit = (lane == sub + 8 * g).astype(f32)
            parts = [gram[at, c : c + 128] for c in range(c0, size, 128)]
            if first:
                parts[0] = jnp.where(lane >= first, parts[0], unit)
            else:
                parts.append(unit)
            tiles.append(parts)
        tiles = eliminate(tiles, first)
        parts = [jnp.concatenate([tile[i] for tile in tiles], axis=0) for i in range(len(tiles[0]))]
        diag_inverse[k] = parts[0] if first else parts.pop()
        lane_b = lax.broadcasted_iota(jnp.int32, (BLK, 128), 1)
        row_b = lax.broadcasted_iota(jnp.int32, (BLK, 128), 0)
        parts[0] = jnp.where(lane_b - first >= row_b, parts[0], 0.0)
        panel = jnp.concatenate(parts, axis=1) if len(parts) > 1 else parts[0]
        if r0 + BLK < size:
            if not first:
                turned = jnp.transpose(parts[0])[BLK:, :]
                at = slice(r0 + BLK, r0 + 2 * BLK)
                gram[at, c0:] = gram[at, c0:] - dot(turned, panel, precision=highest)
            if len(parts) > 1:
                turned = jnp.transpose(parts[1])
                gram[c0 + 128 :, c0 + 128 :] = gram[c0 + 128 :, c0 + 128 :] - dot(turned, parts[1], precision=highest)
        upper[r0 : r0 + BLK, c0:] = panel
        bond[r0 : r0 + BLK, c0:] = jnp.where(mask_pair(r0, BLK, c0), panel, 0.0)
        done(k, r0, c0)


def kernel(
    n, size_list, site, left_env, right_env, left_out, bond_out,
    sizes,    site_v, low_v, left_f, right_f, near_f, cross_f, left_h, left_l, right_h, right_l,
    gram, upper, bond, inv, halo_n, halo_c, app, app_n, app_c, second, part_v, mix_h, mix_l,
    ortho_v, result_v, mine, slots, partner,
    local_sem, out_sem, site_sem, near_sem, cross_sem, bond_sem, app_sem, low_sem, far_sem, pair_sem, known_sem,
):
    me = lax.axis_index("row")
    odd = lax.rem(me, 2)
    size = site.shape[-1]
    half = size // 2
    width = left_env.shape[1]
    own_n = width - HALO
    met_n = own_n + W_DN
    chips = n // 2

    def other(step):
        return {"row": lax.rem(me + step + n, n)}

    near, cross = other(1 - 2 * odd), other(2 * odd - 1)

    def remote(src, dst, sems, target):
        return pltpu.make_async_remote_copy(
            src_ref=src, dst_ref=dst, send_sem=sems.at[0], recv_sem=sems.at[1], device_id=target, device_id_type=MESH
        )

    load_site = pltpu.make_async_copy(site.at[0], site_v, local_sem.at[0])
    load_left = pltpu.make_async_copy(left_env.at[0], left_f, local_sem.at[1])
    load_right = pltpu.make_async_copy(right_env.at[0, pl.ds(HALO, own_n)], right_f, local_sem.at[2])
    load_sizes = pltpu.make_async_copy(size_list, sizes, local_sem.at[3])
    load_site.start()
    load_sizes.start()
    load_left.start()
    load_right.start()

    barrier = pltpu.get_barrier_semaphore()
    for step in (1, -1, 2, -2):
        pl.semaphore_signal(barrier, inc=1, device_id=other(step), device_id_type=MESH)
    pl.semaphore_wait(barrier, 4)

    def env_piece(i, side):
        at = pl.ds(side * half, half)
        return remote(
            right_env.at[0, W_DN * (1 - odd) + i, :, at], cross_f.at[i, :, at], cross_sem.at[side, i], cross
        )

    load_site.wait()
    move_site = remote(site_v.at[1], low_v, site_sem, other(1))
    move_site.start()
    for i in range(W_DN):
        env_piece(i, 0).start()
    move_near = remote(right_env.at[0, pl.ds(W_DN * odd, W_DN)], near_f, near_sem, near)
    move_near.start()

    rounds = []
    reach = 1
    while 2 * reach <= chips // 2:
        rounds.append(reach)
        reach *= 2

    def greet(i):
        if i < len(rounds):
            for step in (2 * rounds[i], -2 * rounds[i]):
                pl.semaphore_signal(known_sem.at[i], inc=1, device_id=other(step), device_id_type=MESH)

    def greeted(i):
        if i < len(rounds):
            pl.semaphore_wait(known_sem.at[i], 2)

    greet(0)

    load_sizes.wait()
    own_size = sizes[me]
    low_size = jnp.where(me == 0, 0, sizes[lax.rem(me + n - 1, n)])

    def mask_pair(r0, rows, c0, c1=size, row_size=None):
        shape = (rows, c1 - c0)
        row = lax.broadcasted_iota(jnp.int32, shape, 0) + r0
        lane = lax.broadcasted_iota(jnp.int32, shape, 1) + c0
        return (row < (own_size if row_size is None else row_size)) & (lane < own_size)

    ortho_v[0] = jnp.where(mask_pair(0, size, 0), site_v[0], 0.0)
    row = lax.broadcasted_iota(jnp.int32, (size, size), 0)
    lane = lax.broadcasted_iota(jnp.int32, (size, size), 1)
    dead = ((row == lane) & (row >= own_size)).astype(f32)
    gram[...] = dot(ortho_v[0], ortho_v[0], ((0,), (0,)), precision=highest) + dead

    def split_right(source, offset):
        def body(i, _):
            at = pl.ds(pl.multiple_of((i + offset) * size, size), size)
            right_h[at, :], right_l[at, :] = split(source[i])
            return 0

        lax.fori_loop(0, source.shape[0], body, 0)

    load_left.wait()

    def split_left(count, source, target):
        def body(i, _):
            left_h[i + target], left_l[i + target] = split(left_f[i + source])
            return 0

        lax.fori_loop(0, count, body, 0)

    split_left(own_n, HALO, 0)
    split_left(W_DN, W_DN * (1 - odd), own_n)
    split_left(W_DN, W_DN * odd, met_n)
    load_right.wait()
    split_right(right_f, 0)
    greeted(0)
    greet(1)

    move_site.wait_recv()
    ortho_v[1] = jnp.where(mask_pair(0, size, 0, size, low_size), low_v[...], 0.0)
    gram[...] = gram[...] + dot(ortho_v[1], ortho_v[1], ((0,), (0,)), precision=highest)
    greeted(1)
    greet(2)

    sends = []

    def bond_piece(k, r0, c0):
        at = (pl.ds(r0, BLK), pl.ds(c0, size - c0))
        for side, (target, halo) in enumerate(((near, halo_n), (cross, halo_c))):
            copy = remote(bond.at[at], halo.at[at], bond_sem.at[side, k], target)
            copy.start()
            sends.append(copy)
        if k == 0:
            env_piece(0, 1).start()
            env_piece(1, 1).start()
        if k == size // BLK - 1:
            env_piece(2, 1).start()
            env_piece(3, 1).start()
            greeted(2)
            greet(3)

    bond[half:, :half] = jnp.zeros((half, half), f32)
    factorize(gram, upper, bond, inv, mask_pair, bond_piece)

    def stage_one(first, last, block):
        high, low = split(block)
        for a in range(first, last):
            at = slice(a * size, (a + 1) * size)
            mix_h[:, at], mix_l[:, at] = split(dot3(left_h[a], left_l[a], high, low))

    def stage_two(first, last, c0=0, c1=size):
        at = slice(first * size, last * size)
        return dot3(mix_h[:, at], mix_l[:, at], right_h[at, c0:c1], right_l[at, c0:c1])

    def bond_halo(ref):
        low = jnp.concatenate([jnp.zeros((half, half), f32), ref[half:, half:]], axis=1)
        return jnp.concatenate([ref[:half, :], low], axis=0)

    at_end = jnp.broadcast_to(lax.rem(me + 1, n), (size, size)) < 2
    has_cross = jnp.logical_not(at_end)

    stage_one(0, own_n, bond[...])
    move_near.wait_recv()
    split_right(near_f, own_n)
    for copy in sends[0::2]:
        copy.wait_recv()
    stage_one(own_n, met_n, bond_halo(halo_n))
    part_v[...] = stage_two(0, met_n)

    def ortho_columns(part, blocks):
        for k in blocks:
            r0 = k * BLK
            c0 = r0 // 128 * 128
            want = ortho_v[part, :, c0 : c0 + 128]
            if k:
                want = want - dot(result_v[part, :, :r0], upper[:r0, c0 : c0 + 128], precision=highest)
            first = r0 - c0
            want = want[:, first : first + BLK]
            result_v[part, :, r0 : r0 + BLK] = dot(want, inv[k][:, :BLK], ((1,), (1,)), precision=highest)

    for copy in sends[1::2]:
        copy.wait_recv()
    stage_one(met_n, width, jnp.where(has_cross, bond_halo(halo_c), 0.0))

    def split_cross(first, last, side):
        at = slice(side * half, (side + 1) * half)
        for i in range(first, last):
            env_piece(i, side).wait_recv()
            rows = slice((met_n + i) * size, (met_n + i + 1) * size)
            right_h[rows, at], right_l[rows, at] = split(cross_f[i, :, at])

    app_sends = []
    for side in range(2):
        c0, c1 = side * half, (side + 1) * half
        total = part_v[:, c0:c1]
        for i in (0, 2) if side else (0,):
            count = 2 if side else W_DN
            split_cross(i, i + count, side)
            total = total + stage_two(met_n + i, met_n + i + count, c0, c1)
        app[:, c0:c1] = jnp.where(mask_pair(0, size, c0, c1), TAU * total, 0.0)
        at = pl.ds(c0, half)
        for to, (target, halo) in enumerate(((cross, app_c), (near, app_n))):
            copy = remote(app.at[:, at], halo.at[:, at], app_sem.at[to, side], target)
            copy.start()
            app_sends.append(copy)

    def total_of(x):
        return jnp.sum(jnp.sum(x, axis=0, keepdims=True), axis=1, keepdims=True)

    stage_one(0, own_n, app[...])
    for copy in app_sends[1::2]:
        copy.wait_recv()
    stage_one(own_n, met_n, app_n[...])
    part_v[...] = stage_two(0, met_n)
    greeted(3)
    for i in range(4, len(rounds)):
        greet(i)
        greeted(i)
    pl.semaphore_signal(known_sem.at[len(rounds)], inc=1, device_id=near, device_id_type=MESH)
    b, a = bond[...], app[...]
    pieces = [total_of(x) for x in (b * b, b * a, a * a)]
    for copy in app_sends[0::2]:
        copy.wait_recv()
    stage_one(met_n, width, jnp.where(has_cross, app_c[...], 0.0))
    second[...] = jnp.where(mask_pair(0, size, 0), (0.5 * TAU) * (part_v[...] + stage_two(met_n, width)), 0.0)
    h = second[...]
    pieces += [total_of(x) for x in (bond[...] * h, app[...] * h, h * h)]
    lane_1 = lax.broadcasted_iota(jnp.int32, (1, 128), 1)
    packed = jnp.zeros((1, 128), f32)
    for i, piece in enumerate(pieces):
        packed = jnp.where(lane_1 == i, piece, packed)
    mine[...] = packed
    pl.semaphore_wait(known_sem.at[len(rounds)], 1)

    def far(d, core):
        slot = (chips - 1) * core + d - 1
        return pltpu.make_async_remote_copy(
            src_ref=mine, dst_ref=slots.at[slot], send_sem=far_sem.at[0, slot], recv_sem=far_sem.at[1, slot],
            device_id={"row": lax.rem(me + 2 * d, n) + core * (1 - 2 * odd)}, device_id_type=MESH,
        )

    swap = remote(mine, partner, pair_sem, near)

    def send_far(i, _):
        d = chips // 2 + (i + 1) // 2 * (2 * (i % 2) - 1)
        far(d, 0).start()
        far(d, 1).start()
        return 0

    lax.fori_loop(0, chips - 1, send_far, 0)
    swap.start()

    ortho_columns(1, range(size // BLK))
    move_low = remote(result_v.at[1], left_out.at[0, 1], low_sem, other(-1))
    move_low.start()
    ortho_columns(0, range(size // BLK))
    store_up = pltpu.make_async_copy(result_v.at[0], left_out.at[0, 0], out_sem.at[0])
    store_up.start()

    def take_far(i, _):
        far(i + 1, 0).wait_recv()
        far(i + 1, 1).wait_recv()
        return 0

    lax.fori_loop(0, chips - 1, take_far, 0)
    swap.wait_recv()
    sums = mine[...] + partner[...] + jnp.sum(slots[...], axis=0)
    bb, ba, aa, bh, ah, hh = (jnp.broadcast_to(sums[:, i : i + 1], (1, size)) for i in range(6))
    step = ba / bb
    weight_b = 1.0 - step + 0.5 * step * step
    weight_a = 1.0 - step
    norm = (
        weight_b * weight_b * bb + 2.0 * weight_b * weight_a * ba + weight_a * weight_a * aa
        + 2.0 * weight_b * bh + 2.0 * weight_a * ah + hh
    )
    scale = jnp.sqrt(bb / norm)
    bond_out[0] = (weight_b * bond[...] + weight_a * app[...] + second[...]) * scale

    def sent_far(i, _):
        far(i + 1, 0).wait_send()
        far(i + 1, 1).wait_send()
        return 0

    lax.fori_loop(0, chips - 1, sent_far, 0)
    pieces = [env_piece(i, side) for i in range(W_DN) for side in range(2)]
    for copy in (move_site, move_near, *pieces, *sends, *app_sends, swap, move_low):
        copy.wait_send()
    move_low.wait_recv()
    store_up.wait()


def store(left, bond, left_out, bond_out, sems):
    copies = [
        pltpu.make_async_copy(left, left_out, sems.at[0]),
        pltpu.make_async_copy(bond, bond_out, sems.at[1]),
    ]
    for copy in copies:
        copy.start()
    for copy in copies:
        copy.wait()


def stored(left, bond):
    here = pl.BlockSpec(memory_space=pltpu.VMEM)
    out = pl.BlockSpec(memory_space=pltpu.HBM)
    return pl.pallas_call(
        store,
        out_shape=(jax.ShapeDtypeStruct(left.shape, f32), jax.ShapeDtypeStruct(bond.shape, f32)),
        in_specs=[here, here],
        out_specs=(out, out),
        scratch_shapes=[pltpu.SemaphoreType.DMA((2,))],
        compiler_params=pltpu.CompilerParams(vmem_limit_bytes=4 * 1024 * 1024),
    )(left, bond)


def on_device(n, site_tensor, left_env, right_env, sector_size):
    size = site_tensor.shape[-1]
    width = left_env.shape[1]
    full = (size, size)
    hbm = pl.BlockSpec(memory_space=pltpu.HBM)
    chips = n // 2
    parts = size // BLK
    scratch = [
        pltpu.SMEM(sector_size.shape, jnp.int32), pltpu.VMEM((2, *full), f32), pltpu.VMEM(full, f32), pltpu.VMEM((width, *full), f32),
        pltpu.VMEM((width - HALO, *full), f32), pltpu.VMEM((W_DN, *full), f32), pltpu.VMEM((W_UP, *full), f32),
        pltpu.VMEM((width, *full), bf16), pltpu.VMEM((width, *full), bf16),
        pltpu.VMEM((width * size, size), bf16), pltpu.VMEM((width * size, size), bf16),
        pltpu.VMEM(full, f32), pltpu.VMEM(full, f32), pltpu.VMEM(full, f32), pltpu.VMEM((parts, BLK, 128), f32),
        *[pltpu.VMEM(full, f32)] * 7,
        pltpu.VMEM((size, width * size), bf16), pltpu.VMEM((size, width * size), bf16),
        pltpu.VMEM((2, *full), f32), pltpu.VMEM((2, *full), f32),
        pltpu.VMEM((1, 128), f32), pltpu.VMEM((2 * chips - 2, 1, 128), f32), pltpu.VMEM((1, 128), f32),
        pltpu.SemaphoreType.DMA((4,)), pltpu.SemaphoreType.DMA((1,)), pltpu.SemaphoreType.DMA((2,)),
        pltpu.SemaphoreType.DMA((2,)), pltpu.SemaphoreType.DMA((2, W_DN, 2)),
        pltpu.SemaphoreType.DMA((2, parts, 2)), pltpu.SemaphoreType.DMA((2, 2, 2)),
        pltpu.SemaphoreType.DMA((2,)), pltpu.SemaphoreType.DMA((2, 2 * chips - 2)), pltpu.SemaphoreType.DMA((2,)),
        pltpu.SemaphoreType.REGULAR((max(1, chips.bit_length()),)),
    ]
    left, bond = pl.pallas_call(
        functools.partial(kernel, n),
        out_shape=(
            jax.ShapeDtypeStruct((1, 2, *full), f32),
            jax.ShapeDtypeStruct((1, *full), f32),
        ),
        in_specs=[hbm, hbm, hbm, hbm],
        out_specs=(hbm, pl.BlockSpec(memory_space=pltpu.VMEM)),
        scratch_shapes=scratch,
        compiler_params=pltpu.CompilerParams(
            collective_id=0, has_side_effects=True, vmem_limit_bytes=53 * 1024 * 1024
        ),
    )(pltpu.with_memory_space_constraint(sector_size, pltpu.HBM), site_tensor, left_env, right_env)
    return stored(left, bond)


def solution(mesh):
    block = P(("real", "row"), None, None, None)
    return jax.shard_map(
        functools.partial(on_device, mesh.shape["row"]),
        mesh=mesh,
        in_specs=(block, block, block, P("real")),
        out_specs=(block, P(("real", "row"), None, None)),
        check_vma=False,
    )
```
